256 devices in a mesh: groups: 4 (over y, x), sph: 64 (over z, core).
Axes of the slice: x: 2, y: 2, z: 32, core: 2. Of those that a mesh axis runs over, the one named last changes fastest.
The devices are a block of a 4x8x32 slice.
Arguments:
- positions: float32 [2048, 3], P('sph'), may hold values from -8 to 8
- wave_vectors: float32 [256, 3], replicated, may hold values from -5 to 5
- pattern: float32 [2, 448, 256], replicated, may hold values from -6 to 6
- dir_index: int32 [128], P('groups'), parts along dimension 0, may hold values from 0 to 255
- mie: float32 [2, 448, 2048], P(None, None, 'sph'), may hold values from -0.9 to 0.9
- trans_table: bfloat16 [8, 2, 448, 448], replicated, may hold values from -0.1875 to 0.1875
- pair_route: int32 [4096, 1], P('sph'), may hold values from 0 to 63; in each aligned block of 64 rows (0 to 63, 64 to 127, ...) at most 2 rows name the same one
- pair_source: int32 [4096], P('sph'), may hold values from 0 to 15
- pair_target: int32 [4096], P('sph'), may hold values from 0 to 15
- pair_class: int32 [4096], P('sph'), may hold values from 0 to 7
Outputs:
- scattered: bfloat16 [896, 262144], P(None, ('groups', 'sph')), parts along dimension 1
- extinction: float32 [128], P('groups'), parts along dimension 0
The draws below stay inside these ranges and needn't reach their ends.
There are 4 independent parts, one for each index of `groups`. The reference program is written for one: setup_inputs(seed, part) draws one part's arguments, and reference() takes and returns one part's arrays. A program takes and returns all parts, laid end to end along the dimension named above; an argument that names none is the same for every part. Nothing has to cross between parts.
Inputs may be any that keep to these rules, and one draw needn't show every extreme that they name: `pair_route`: among the rows of one device no device is named by more than 2 pairs, and in every draw some device is named by exactly 2 of them.
All inputs are finite; a program needn't handle non-finite values.
Results may differ from the reference program's by a relative error of at most 0.0051.
Values may be sent and summed in bfloat16 or wider, within the bound.
A program may use at most 192 MiB of HBM per device.

```python
import math
import jax
import jax.numpy as jnp
import numpy as np
from jax import lax

MODES = 448
DIRS = 32
DIRTAB = 256
CLASSES = 8
BLOCK = 2
BLK_DEV = 16
PAIRS_DEV = 64
CAP = 2
SPHERES = 2048
PAIRS = 4096
N_SPH = 64


def place_ends(drawn, key, smallest, high):
    extent = drawn.shape
    index_at = [jax.random.randint(jax.random.fold_in(key, axis), (), 0, extent[axis]) for axis in range(len(extent))]
    drawn = drawn.at[tuple(index_at)].set(smallest)
    longest = extent.index(max(extent))
    index_at[longest] = (index_at[longest] + 1) % extent[longest]
    return drawn.at[tuple(index_at)].set(high)


def shard_levels(stream_key, shape, shards, smallest, top_value):
    factor_of = 1.0
    for axis_at, shards_of in shards:
        heights = jax.random.uniform(jax.random.fold_in(jax.random.fold_in(stream_key, 6), axis_at), (shards_of,), jnp.float32, smallest / len(shards), top_value / len(shards))
        factor_of = factor_of * jnp.repeat(jnp.exp(heights), shape[axis_at] // shards_of).reshape((-1,) + (1,) * (len(shape) - 1 - axis_at))
    return factor_of


def shared_out(own_key, own, number, rows, number_of, top, bound, lean):
    order = jax.random.permutation(own_key, number_of)
    crowded, common = load_shares(number_of, rows * top, bound, lean, True), load_shares(number_of, rows * top, bound, lean, False)
    places = jnp.arange(number_of)

    def named(tallies, offset_by):
        used = int((tallies > 0).sum())
        fixed = max(1, used // 4)
        shifted = fixed + (places - fixed + offset_by * (used - fixed)) % max(1, number_of - fixed)
        return jnp.zeros((number_of,), jnp.int32).at[order[jnp.where(places < fixed, places, shifted)]].set(jnp.asarray(tallies, jnp.int32))

    tallies = jnp.where(number % 4 == 0, named(crowded, number // 4), named(common, number - number // 4 - 1))
    mixed = jax.random.permutation(jax.random.fold_in(own, 3), number_of)
    giver, sink = mixed[0:number_of // 2 * 2:2], mixed[1:number_of // 2 * 2:2]
    slack = jnp.minimum(tallies[giver] - 1, bound - tallies[sink]) // 2
    slack = jnp.where((giver == order[0]) | (sink == order[0]) | (tallies[sink] == 0), 0, jnp.maximum(slack, 0))
    shifted = jax.random.randint(jax.random.fold_in(own, 4), (number_of // 2,), 0, 1 << 20) % (slack + 1)
    tallies = tallies.at[giver].add(-shifted).at[sink].add(shifted)
    items = jnp.searchsorted(jnp.cumsum(tallies), jnp.arange(rows * top), side="right").astype(jnp.int32)
    table = items.reshape(top, rows).T
    table = table[jax.random.permutation(jax.random.fold_in(own, 1), rows)]
    offset_by = jax.random.randint(jax.random.fold_in(own, 2), (rows, 1), 0, top)
    return jnp.take_along_axis(table, (jnp.arange(top)[None, :] + offset_by) % top, axis=1)


def load_shares(count, total, bound, skew, full):
    portions = [(1 << 20) // math.isqrt(rank ** skew) + 1 for rank in range(1, count + 1)]
    largest = bound if full else min(bound, max(-(-total // count), total * portions[0] // sum(portions)))
    least = 1 if total - largest >= count - 1 else 0
    given, rest = [largest] + [least] * (count - 1), total - largest - least * (count - 1)
    while rest > 0:
        candidates = [i for i in range(1, count) if given[i] < largest] or [i for i in range(1, count) if given[i] < bound]
        pool, budget = sum([portions[i] for i in candidates]), rest
        for i in candidates:
            addition = min(bound - given[i], max(1, budget * portions[i] // pool), rest)
            given[i] = given[i] + addition
            rest = rest - addition
    return np.array(given)


def gaussian(key, shape, scale, most, kind=jnp.bfloat16):
    return jnp.clip(scale * jax.random.normal(key, shape, jnp.float32), -most, most).astype(kind)


def setup_inputs(seed: int = 0, part: int = 0) -> dict:
    key_list = jax.random.split(jax.random.key(seed), 11)
    part_splits = jax.random.split(jax.random.fold_in(key_list[10], part), 11)
    positions = jnp.clip(jax.random.uniform(key_list[0], (SPHERES, 3), jnp.float32, -8.0, 8.0) * shard_levels(key_list[0], (SPHERES, 3), ((0, 64),), -0.4, 0.0), -8.0, 8.0)
    wave_vectors = gaussian(key_list[1], (DIRTAB, 3), 1.0, 5.0, jnp.float32)
    pattern = gaussian(key_list[2], (2, MODES, DIRTAB), 1.0, 6.0, jnp.float32)
    dir_index = place_ends(jax.random.randint(part_splits[3], (DIRS,), 0, DIRTAB), jax.random.fold_in(part_splits[3], 1), 0, DIRTAB - 1).astype(jnp.int32)
    mie = jnp.clip(jax.random.uniform(key_list[4], (2, MODES, SPHERES), jnp.float32, -0.9, 0.9) * shard_levels(key_list[4], (2, MODES, SPHERES), ((2, 64),), -0.4, 0.0), -0.9, 0.9)
    trans_table = gaussian(key_list[5], (CLASSES, 2, MODES, MODES), (2 * MODES) ** -0.5, 0.1875)
    pair_route_keys = jax.random.split(jax.random.fold_in(key_list[6], 1), PAIRS // PAIRS_DEV)
    pair_route_turns = jax.random.permutation(jax.random.fold_in(key_list[6], 3), PAIRS // PAIRS_DEV)
    pair_route = jax.vmap(lambda own, number: shared_out(jax.random.fold_in(key_list[6], 2), own, number, PAIRS_DEV, N_SPH, 1, CAP, 2))(pair_route_keys, pair_route_turns).reshape((PAIRS, 1))
    pair_source = place_ends(jax.random.randint(key_list[7], (PAIRS,), 0, BLK_DEV), jax.random.fold_in(key_list[7], 1), 0, BLK_DEV - 1).astype(jnp.int32)
    pair_target = place_ends(jax.random.randint(key_list[8], (PAIRS,), 0, BLK_DEV), jax.random.fold_in(key_list[8], 1), 0, BLK_DEV - 1).astype(jnp.int32)
    pair_class = place_ends(jax.random.randint(key_list[9], (PAIRS,), 0, CLASSES), jax.random.fold_in(key_list[9], 1), 0, CLASSES - 1).astype(jnp.int32)
    return dict(positions=positions, wave_vectors=wave_vectors, pattern=pattern, dir_index=dir_index, mie=mie, trans_table=trans_table, pair_route=pair_route, pair_source=pair_source, pair_target=pair_target, pair_class=pair_class)


def reference(positions, wave_vectors, pattern, dir_index, mie, trans_table, pair_route, pair_source, pair_target, pair_class):
    directions = wave_vectors[dir_index]
    phases = positions[:, 0:1] * directions[None, :, 0] + positions[:, 1:2] * directions[None, :, 1] + positions[:, 2:3] * directions[None, :, 2]
    cosine = jnp.cos(phases)
    sine_part = jnp.sin(phases)
    chosen = pattern[:, :, dir_index]
    inc_real = cosine[None] * chosen[0][:, None, :] - sine_part[None] * chosen[1][:, None, :]
    inc_imag = cosine[None] * chosen[1][:, None, :] + sine_part[None] * chosen[0][:, None, :]
    mie_real = mie[0][:, :, None]
    mie_imag = mie[1][:, :, None]
    scat_real = mie_real * inc_real - mie_imag * inc_imag
    scat_imag = mie_real * inc_imag + mie_imag * inc_real
    coeffs = jnp.concatenate([scat_real, scat_imag], 0).astype(jnp.bfloat16)
    columns = BLOCK * DIRS
    block_count = SPHERES // BLOCK
    block_data = coeffs.reshape(2 * MODES, block_count, columns).transpose(1, 0, 2)
    owner = jnp.arange(PAIRS, dtype=jnp.int32) // PAIRS_DEV
    source_global = (owner * BLK_DEV + pair_source).astype(jnp.int32)
    target_global = (pair_route[:, 0] * BLK_DEV + pair_target).astype(jnp.int32)
    group_shape = (PAIRS // 8, 8)

    def add_group(field_sum, group_items):
        sources, targets, classes = group_items
        tables = trans_table[classes].astype(jnp.float32)
        values = block_data[sources].astype(jnp.float32)
        data_real = values[:, :MODES]
        data_imag = values[:, MODES:]
        highest = lax.Precision.HIGHEST
        part_real = jnp.einsum('kij,kjc->kic', tables[:, 0], data_real, precision=highest) - jnp.einsum('kij,kjc->kic', tables[:, 1], data_imag, precision=highest)
        part_imag = jnp.einsum('kij,kjc->kic', tables[:, 1], data_real, precision=highest) + jnp.einsum('kij,kjc->kic', tables[:, 0], data_imag, precision=highest)
        contribution = jnp.concatenate([part_real, part_imag], 1).astype(jnp.bfloat16)
        contribution = lax.optimization_barrier(contribution).astype(jnp.float32)
        return field_sum.at[targets].add(contribution), None

    initial = jnp.zeros((block_count, 2 * MODES, columns), jnp.float32)
    summed, unused = lax.scan(add_group, initial, (source_global.reshape(group_shape), target_global.reshape(group_shape), pair_class.astype(jnp.int32).reshape(group_shape)))
    summed = summed.transpose(1, 0, 2).reshape(2 * MODES, SPHERES, DIRS)
    total_real = inc_real + summed[:MODES]
    total_imag = inc_imag + summed[MODES:]
    out_real = mie_real * total_real - mie_imag * total_imag
    out_imag = mie_real * total_imag + mie_imag * total_real
    scattered = jnp.concatenate([out_real, out_imag], 0).reshape(2 * MODES, SPHERES * DIRS).astype(jnp.bfloat16)
    extinction = jnp.sum(inc_real * out_real + inc_imag * out_imag, axis=(0, 1))
    return (scattered, extinction)
```

```python
import functools

import jax
import jax.numpy as jnp
from jax import lax
from jax.experimental import pallas as pl
from jax.experimental.pallas import tpu as pltpu
from jax.sharding import PartitionSpec as P

BLOCK = 2
LANES = 128
F32 = jnp.float32
BF16 = jnp.bfloat16
HIGHEST = lax.Precision.HIGHEST
NT = (((1,), (1,)), ((), ()))


def iota(shape, axis):
    return lax.broadcasted_iota(jnp.int32, shape, axis)


def split3(x):
    hi = x.astype(BF16)
    rest = x - hi.astype(F32)
    mid = rest.astype(BF16)
    low = (rest - mid.astype(F32)).astype(BF16)
    return hi, mid, low


def pack_kernel(mie_ref, pos_ref, route_ref, source_ref, target_ref, class_ref, out_ref):
    dests = out_ref.shape[1]
    pairs = route_ref.shape[1]
    spheres = pos_ref.shape[0]
    named = (route_ref[...] == iota((dests, pairs), 0)).astype(BF16)
    earlier = (iota((pairs, pairs), 0) < iota((pairs, pairs), 1)).astype(BF16)
    before = jnp.dot(named, earlier, preferred_element_type=F32)
    pos = pos_ref[...]
    hi, mid, low = (part.astype(F32) for part in split3(pos))
    lane = iota(pos.shape, 1)
    pos_parts = jnp.where(lane < 3, hi, jnp.where(lane < 6, mid, low)).astype(BF16)
    row = iota((LANES, pairs), 0)
    pair_meta = jnp.where(
        row == 9, target_ref[...] + 1, jnp.where(row == 10, class_ref[...], 0)
    ).astype(F32).astype(BF16)
    for r in range(2):
        slot = jnp.where(before == float(r), named.astype(F32), 0.0).astype(BF16)
        meta = lax.dot_general(slot, pair_meta, NT, preferred_element_type=F32)
        for s in range(2):
            origin = (source_ref[...] * BLOCK + s == iota((spheres, pairs), 0)).astype(F32).astype(BF16)
            pick = lax.dot_general(slot, origin, NT, preferred_element_type=F32).astype(BF16)
            where = jnp.dot(pick, pos_parts, preferred_element_type=F32)
            units = mie_ref.shape[0] // LANES
            for u in range(units):
                rows = mie_ref[u * LANES : (u + 1) * LANES, :].astype(BF16)
                out_ref[2 * r + s, :, u, :] = lax.dot_general(pick, rows, NT, preferred_element_type=F32).astype(BF16)
            out_ref[2 * r + s, :, units, :] = (where + meta).astype(BF16)


def field_kernel(
    slots_ref, pattern_ref, wave_ref, dirs_ref, own_ref, mie_ref, table_ref, out_ref, ext_ref,
    left, weights, x_buf, z_buf, pat, mie_wide,
):
    modes = table_ref.shape[2]
    both = 2 * modes
    sources = slots_ref.shape[1]
    slots = 2 * sources
    columns = out_ref.shape[1]
    half = columns // 2
    classes = table_ref.shape[0]
    dirs = LANES // 4
    select = (iota((pattern_ref.shape[1], LANES), 0) == dirs_ref[...]).astype(F32)
    pat[...] = jnp.dot(pattern_ref[...], select, precision=HIGHEST, preferred_element_type=F32)
    waves = jnp.dot(wave_ref[...], select, precision=HIGHEST, preferred_element_type=F32)
    kx, ky, kz = waves[0:1], waves[1:2], waves[2:3]

    wide = iota((mie_ref.shape[1], columns), 1)
    sphere_of = (wide // dirs) % (half // dirs) * BLOCK + wide // half
    spread = (iota(wide.shape, 0) == sphere_of).astype(F32).astype(BF16)
    total = None
    for part in split3(mie_ref[...]):
        term = jnp.dot(part, spread, preferred_element_type=F32)
        total = term if total is None else total + term
    mie_wide[...] = total

    units = both // LANES
    phases = []
    for s in range(2):
        for u in range(units):
            block = jnp.concatenate(
                [slots_ref[s, :, u, :].astype(F32), slots_ref[2 + s, :, u, :].astype(F32)], 0
            )
            left[s, u * LANES : (u + 1) * LANES, 0:slots] = block.T.astype(BF16)
        left[s, 0:modes, slots : 2 * slots] = -left[s, modes:both, 0:slots]
        left[s, modes:both, slots : 2 * slots] = left[s, 0:modes, 0:slots]
        meta = jnp.concatenate(
            [slots_ref[s, :, units, :].astype(F32), slots_ref[2 + s, :, units, :].astype(F32)], 0
        )
        x = meta[:, 0:1] + meta[:, 3:4] + meta[:, 6:7]
        y = meta[:, 1:2] + meta[:, 4:5] + meta[:, 7:8]
        z = meta[:, 2:3] + meta[:, 5:6] + meta[:, 8:9]
        phase = x * kx + y * ky + z * kz
        phases.append((jnp.cos(phase), jnp.sin(phase)))
        code = meta[:, 10:11] * float(half // dirs) + meta[:, 9:10] - 1.0
        code = jnp.where(meta[:, 9:10] > 0.0, code, -1.0)
    code = jnp.broadcast_to(code, (slots, LANES))

    def one_class(c, carry):
        for s in range(2):
            cosine, sine = phases[s]
            for t in range(half // LANES):
                block_of = (iota((slots, LANES), 1) // dirs + t * (LANES // dirs) + c * (half // dirs)).astype(F32)
                hit = code == block_of
                weights[0:slots, t * LANES : (t + 1) * LANES] = jnp.where(hit, cosine, 0.0).astype(BF16)
                weights[slots : 2 * slots, t * LANES : (t + 1) * LANES] = jnp.where(hit, sine, 0.0).astype(BF16)
            for n in range(half // 256):
                cut = slice(n * 256, (n + 1) * 256)
                gathered = jnp.dot(left[s], weights[:, cut], preferred_element_type=F32)
                for t in range(2):
                    lanes = slice(t * LANES, (t + 1) * LANES)
                    g_real, g_imag = gathered[:modes, lanes], gathered[modes:, lanes]
                    p_real, p_imag = pat[:modes, :], pat[modes:, :]
                    at = s * half + n * 256 + t * LANES
                    x_buf[:, at : at + LANES] = (g_real * p_real - g_imag * p_imag).astype(BF16)
                    x_buf[:, columns + at : columns + at + LANES] = (g_real * p_imag + g_imag * p_real).astype(BF16)
        matrix = table_ref[c].reshape(both, modes)

        def one_cut(n, carry):
            at = pl.ds(pl.multiple_of(n * 512, 512), 512)
            z_buf[:, at] += jnp.dot(matrix, x_buf[:, at], preferred_element_type=F32)
            return carry

        return lax.fori_loop(0, 2 * columns // 512, one_cut, carry)

    z_buf[...] = jnp.zeros_like(z_buf)
    lax.fori_loop(0, classes, one_class, 0)

    order_in, order_out = iota((256, 256), 0), iota((256, 256), 1)
    wanted = (order_out // dirs) % 2 * LANES + order_out // (2 * dirs) * dirs + order_out % dirs
    shuffle = (order_in == wanted).astype(F32).astype(BF16)
    ext = jnp.zeros((8, LANES), F32)
    for t in range(half // LANES):
        parts = []
        for s in range(2):
            at = s * half + t * LANES
            lanes = slice(at, at + LANES)
            own = slice(columns + at, columns + at + LANES)
            phase = own_ref[0:1, lanes] * kx + own_ref[1:2, lanes] * ky + own_ref[2:3, lanes] * kz
            cosine, sine = jnp.cos(phase), jnp.sin(phase)
            p_real, p_imag = pat[:modes, :], pat[modes:, :]
            inc_real = cosine * p_real - sine * p_imag
            inc_imag = cosine * p_imag + sine * p_real
            tot_real = inc_real + (z_buf[:modes, lanes] - z_buf[modes:, own])
            tot_imag = inc_imag + (z_buf[modes:, lanes] + z_buf[:modes, own])
            m_real, m_imag = mie_wide[:modes, lanes], mie_wide[modes:, lanes]
            o_real = m_real * tot_real - m_imag * tot_imag
            o_imag = m_real * tot_imag + m_imag * tot_real
            ext += (inc_real * o_real + inc_imag * o_imag).reshape(modes // 8, 8, LANES).sum(0)
            parts.append((o_real.astype(BF16), o_imag.astype(BF16)))
        out = slice(t * 256, (t + 1) * 256)
        for k in range(2):
            mixed = jnp.concatenate([parts[0][k], parts[1][k]], 1)
            out_ref[k * modes : (k + 1) * modes, out] = jnp.dot(
                mixed, shuffle, preferred_element_type=F32
            ).astype(BF16)
    ext_ref[...] = ext


def shards(
    positions, wave_vectors, pattern, dir_index, mie, trans_table, pair_route, pair_source, pair_target, pair_class,
):
    modes = pattern.shape[1]
    spheres = positions.shape[0]
    dirs = dir_index.shape[0]
    devices = lax.axis_size("sph")
    groups = lax.axis_size("groups")
    pairs = pair_source.shape[0]
    columns = spheres * dirs
    units = 2 * modes // LANES + 1
    mie = mie.reshape(2 * modes, spheres)
    pattern = pattern.reshape(2 * modes, -1)
    pos_wide = jnp.pad(jnp.concatenate([positions] * 3, 1), ((0, 0), (0, LANES - 9)))
    wave_rows = jnp.pad(wave_vectors.T, ((0, 5), (0, 0)))
    dir_row = jnp.tile(dir_index, LANES // dirs)[None]
    own = jnp.broadcast_to(
        positions.reshape(spheres // BLOCK, BLOCK, 3).transpose(2, 1, 0)[..., None], (3, BLOCK, spheres // BLOCK, dirs)
    ).reshape(3, columns)
    own = jnp.pad(own, ((0, 5), (0, 0)))
    vmem = pl.BlockSpec(memory_space=pltpu.VMEM)
    packed = pl.pallas_call(
        pack_kernel,
        out_shape=jax.ShapeDtypeStruct((4, devices, units, LANES), BF16),
        in_specs=[vmem] * 6,
        out_specs=vmem,
        name="pack",
    )(mie, pos_wide, pair_route.reshape(1, pairs), pair_source[None], pair_target[None], pair_class[None])
    share = packed.transpose(1, 0, 2, 3).reshape(devices, groups, 4 * units * LANES // groups)
    share = lax.dynamic_index_in_dim(share, lax.axis_index("groups"), 1, keepdims=False)
    arrived = lax.all_to_all(share, "sph", split_axis=0, concat_axis=0, tiled=True)
    slots = lax.all_gather(arrived, "groups", axis=1, tiled=False)
    slots = slots.reshape(devices, 4, units, LANES).transpose(1, 0, 2, 3)
    scattered, ext = pl.pallas_call(
        field_kernel,
        out_shape=(
            jax.ShapeDtypeStruct((2 * modes, columns), BF16),
            jax.ShapeDtypeStruct((8, LANES), F32),
        ),
        in_specs=[vmem] * 7,
        out_specs=(vmem, vmem),
        scratch_shapes=[
            pltpu.VMEM((2, 2 * modes, 4 * devices), BF16),
            pltpu.VMEM((4 * devices, columns // 2), BF16),
            pltpu.VMEM((modes, 2 * columns), BF16),
            pltpu.VMEM((2 * modes, 2 * columns), F32),
            pltpu.VMEM((2 * modes, LANES), F32),
            pltpu.VMEM((2 * modes, columns), F32),
        ],
        compiler_params=pltpu.CompilerParams(vmem_limit_bytes=60 * 1024 * 1024),
        name="field",
    )(slots, pattern, wave_rows, dir_row, own, mie, trans_table)
    local = ext.sum(0).reshape(LANES // dirs, dirs).sum(0)
    copies = jnp.broadcast_to(local, (devices, dirs))
    extinction = lax.all_to_all(copies, "sph", split_axis=0, concat_axis=0, tiled=True).sum(0)
    return (scattered, extinction)


def solution(mesh):
    placed = (
        P("sph", None),
        P(),
        P(),
        P("groups"),
        P(None, None, "sph"),
        P(),
        P("sph", None),
        P("sph"),
        P("sph"),
        P("sph"),
    )
    return jax.shard_map(
        shards,
        mesh=mesh,
        in_specs=placed,
        out_specs=(P(None, ("groups", "sph")), P("groups")),
        check_vma=False,
    )
```

```python
import jax
import jax.numpy as jnp
from jax import lax
from jax.experimental import pallas as pl
from jax.experimental.pallas import tpu as pltpu
from jax.sharding import PartitionSpec as P

BLOCK = 2
LANES = 128
WIDE = 256
PART = 8
TARGET_AT = 24
CLASS_AT = 25
F32 = jnp.float32
BF16 = jnp.bfloat16
HIGHEST = lax.Precision.HIGHEST
MESH = pl.DeviceIdType.MESH
NT = (((1,), (1,)), ((), ()))


def iota(shape, axis):
    return lax.broadcasted_iota(jnp.int32, shape, axis)


def ones_where(mask):
    return mask.astype(F32).astype(BF16)


def split3(x):
    hi = x.astype(BF16)
    rest = x - hi.astype(F32)
    mid = rest.astype(BF16)
    low = (rest - mid.astype(F32)).astype(BF16)
    return hi, mid, low


def dot(a, b, **kw):
    return jnp.dot(a, b, preferred_element_type=F32, **kw)


def body(
    route_ref, source_ref, target_ref, class_ref, pos_ref, wave_ref, dirs_ref, mie_ref, pattern_ref, table_hbm,
    out_ref, ext_ref,
    send, recv, ext_send, ext_recv, table, table_sem, send_sem, recv_sem, gsend_sem, grecv_sem, esend_sem, erecv_sem,
    parts, mie_rows, pat, mie_wide, inc, base, left, weights, matrix, x_all,
):
    me = lax.axis_index("sph")
    group = lax.axis_index("groups")
    devices = lax.axis_size("sph")
    groups = lax.axis_size("groups")
    pairs = route_ref.shape[1]
    spheres, modes = mie_ref.shape[1:]
    both = 2 * modes
    classes = table.shape[0]
    columns = out_ref.shape[1]
    dirs = dirs_ref.shape[1]
    blocks = spheres // BLOCK
    tile_blocks = LANES // dirs
    tiles = blocks // tile_blocks
    slots = 2 * devices
    units = both // LANES + 1
    share = recv.shape[2]
    whole = modes // LANES

    barrier = pltpu.get_barrier_semaphore()

    def greet(i, carry):
        pl.semaphore_signal(barrier, inc=1, device_id={"sph": lax.rem(me + i, devices)}, device_id_type=MESH)
        return carry

    def greet_group(i, carry):
        pl.semaphore_signal(barrier, inc=1, device_id={"groups": lax.rem(group + i, groups)}, device_id_type=MESH)
        return carry

    lax.fori_loop(1, devices, greet, 0)
    lax.fori_loop(1, groups, greet_group, 0)
    load_table = pltpu.make_async_copy(table_hbm, table, table_sem)
    load_table.start()

    named = ones_where(route_ref[...] == iota((devices, pairs), 0))
    earlier = ones_where(iota((pairs, pairs), 0) < iota((pairs, pairs), 1))
    before = dot(named, earlier)
    parts[...] = jnp.zeros_like(parts)
    for i, part in enumerate(split3(pos_ref[...])):
        parts[i * PART : i * PART + 3, :] = part.astype(F32)
    row = iota((LANES, pairs), 0)
    pair_meta = jnp.where(
        row == TARGET_AT, target_ref[...] + 1, jnp.where(row == CLASS_AT, class_ref[...], 0)
    ).astype(F32).astype(BF16)
    mixed = jnp.concatenate([mie_ref[0, :, whole * LANES :], mie_ref[1, :, whole * LANES :]], 1)
    first_unit = group * share
    rows_of_share = max(1, share // units)
    for n in range(rows_of_share):
        kind = first_unit // units + n
        rank = (kind // 2).astype(F32)
        sphere = lax.rem(kind, 2)
        slot = jnp.where(before == rank, named.astype(F32), 0.0).astype(BF16)
        origin = ones_where(source_ref[...] * BLOCK + sphere == iota((spheres, pairs), 0))
        pick = lax.dot_general(slot, origin, NT, preferred_element_type=F32).astype(BF16)
        meta = lax.dot_general(slot, pair_meta, NT, preferred_element_type=F32)
        where = lax.dot_general(pick, parts[...].astype(BF16), NT, preferred_element_type=F32)
        for u in range(units):
            if u == units - 1:
                value = where + meta
            else:
                c, t = divmod(u, whole)
                rows = mixed if c == 2 else mie_ref[c, :, t * LANES : (t + 1) * LANES]
                value = dot(pick, rows.astype(BF16))
            at = n * units + u
            send[at // share, :, at % share, :] = value.astype(BF16)
    piece = lax.rem(first_unit, units) // share if share < units else 0

    pl.semaphore_wait(barrier, devices + groups - 2)

    def offset_of(i):
        return devices // 2 + (i + 1) // 2 * (1 - 2 * lax.rem(i, 2))

    def exchange(src, dst, sends, receives, offset):
        return pltpu.make_async_remote_copy(
            src_ref=src,
            dst_ref=dst,
            send_sem=sends.at[offset],
            recv_sem=receives.at[offset],
            device_id={"sph": lax.rem(me + offset, devices)},
            device_id_type=MESH,
        )

    def slot_copy(i, landing):
        offset = offset_of(i)
        to = lax.rem(me + offset, devices)
        here = lax.rem(me + devices - offset, devices) if landing else me
        return exchange(send.at[piece, to], recv.at[group, here], send_sem, recv_sem, offset)

    def start_slot(i, carry):
        slot_copy(i, False).start()
        return carry

    lax.fori_loop(0, devices - 1, start_slot, 0)
    recv[group, me] = send[piece, me]

    lane_dir = dirs_ref[...]
    lane_dirs = jnp.concatenate([lane_dir] * tile_blocks, 1)
    select = (iota((pattern_ref.shape[1], LANES), 0) == lane_dirs).astype(F32)
    pat[...] = dot(pattern_ref[...], select, precision=HIGHEST)
    waves = dot(wave_ref[...], select, precision=HIGHEST)
    kx, ky, kz = waves[0:1], waves[1:2], waves[2:3]
    wide = iota((LANES, columns), 1)
    sphere_of = ((wide // WIDE) * tile_blocks + wide // dirs % tile_blocks) * BLOCK + wide // LANES % BLOCK
    spread = ones_where(lax.rem(iota((LANES, columns), 0), spheres) == sphere_of)
    own = dot(pos_ref[...], spread[0:spheres].astype(F32), precision=HIGHEST)
    mie_rows[...] = jnp.zeros_like(mie_rows)
    for c in range(2):
        for i, part in enumerate(split3(mie_ref[c])):
            mie_rows[i * spheres : (i + 1) * spheres, 0:modes] = part.astype(F32)
        mie_wide[c * modes : (c + 1) * modes, :] = dot(mie_rows[...].T[:modes].astype(BF16), spread)
    for n in range(columns // LANES):
        lanes = slice(n * LANES, (n + 1) * LANES)
        phase = own[0:1, lanes] * kx + own[1:2, lanes] * ky + own[2:3, lanes] * kz
        cosine, sine = jnp.cos(phase), jnp.sin(phase)
        p_real, p_imag = pat[:modes, :], pat[modes:, :]
        i_real = cosine * p_real - sine * p_imag
        i_imag = cosine * p_imag + sine * p_real
        m_real, m_imag = mie_wide[:modes, lanes], mie_wide[modes:, lanes]
        inc[:modes, lanes] = i_real
        inc[modes:, lanes] = i_imag
        base[:modes, lanes] = m_real * i_real - m_imag * i_imag
        base[modes:, lanes] = m_real * i_imag + m_imag * i_real
    load_table.wait()
    for c in range(classes // 2):
        matrix[:, c * both : (c + 1) * both] = jnp.concatenate([table[2 * c], table[2 * c + 1]], 1)

    def end_slot(i, carry):
        copy = slot_copy(i, True)
        copy.wait_send()
        copy.wait_recv()
        return carry

    lax.fori_loop(0, devices - 1, end_slot, 0)

    def share_copy(i, landing):
        at = lax.rem(group + groups - i, groups) if landing else group
        return pltpu.make_async_remote_copy(
            src_ref=recv.at[group],
            dst_ref=recv.at[at],
            send_sem=gsend_sem.at[i],
            recv_sem=grecv_sem.at[i],
            device_id={"groups": lax.rem(group + i, groups)},
            device_id_type=MESH,
        )

    def start_share(i, carry):
        share_copy(i, False).start()
        return carry

    def end_share(i, carry):
        copy = share_copy(i, True)
        copy.wait_send()
        copy.wait_recv()
        return carry

    lax.fori_loop(1, groups, start_share, 0)
    lax.fori_loop(1, groups, end_share, 0)

    def arrived(s, u):
        both_ranks = []
        for r in range(2):
            at = (2 * r + s) * units + u
            both_ranks.append(recv[at // share, :, at % share, :].astype(F32))
        return jnp.concatenate(both_ranks, 0)

    phases = []
    for s in range(2):
        for u in range(units - 1):
            c, t = divmod(u, whole)
            block = arrived(s, u).T.astype(BF16)
            if c < 2:
                at = c * modes + t * LANES
                left[s, at : at + LANES, 0:slots] = block
            else:
                rest = modes - whole * LANES
                left[s, whole * LANES : modes, 0:slots] = block[:rest]
                left[s, modes + whole * LANES : both, 0:slots] = block[rest:]
        left[s, 0:modes, slots : 2 * slots] = -left[s, modes:both, 0:slots]
        left[s, modes:both, slots : 2 * slots] = left[s, 0:modes, 0:slots]
        meta = arrived(s, units - 1)
        x, y, z = (
            meta[:, i : i + 1] + meta[:, PART + i : PART + i + 1] + meta[:, 2 * PART + i : 2 * PART + i + 1]
            for i in range(3)
        )
        phase = x * kx + y * ky + z * kz
        phases.append((jnp.cos(phase), jnp.sin(phase)))
    target = meta[:, TARGET_AT : TARGET_AT + 1]
    code = jnp.where(target > 0.0, meta[:, CLASS_AT : CLASS_AT + 1] * float(blocks) + target - 1.0, -1.0)
    code = jnp.broadcast_to(code, (slots, LANES))

    def form(c, carry):
        rows = pl.ds(pl.multiple_of(c * modes, 64), modes)
        for s in range(2):
            cosine, sine = phases[s]
            for t in range(tiles):
                block_of = (iota((slots, LANES), 1) // dirs + t * tile_blocks + c * blocks).astype(F32)
                hit = code == block_of
                lanes = slice(t * LANES, (t + 1) * LANES)
                weights[s, 0:slots, lanes] = jnp.where(hit, cosine, 0.0).astype(BF16)
                weights[s, slots : 2 * slots, lanes] = jnp.where(hit, sine, 0.0).astype(BF16)
        for s in range(2):
            for n in range(tiles // 2):
                gathered = dot(left[s], weights[s, :, n * WIDE : (n + 1) * WIDE])
                for t in range(2):
                    lanes = slice(t * LANES, (t + 1) * LANES)
                    g_real, g_imag = gathered[:modes, lanes], gathered[modes:, lanes]
                    p_real, p_imag = pat[:modes, :], pat[modes:, :]
                    at = (2 * n + t) * WIDE + s * LANES
                    x_all[0, rows, at : at + LANES] = (g_real * p_real - g_imag * p_imag).astype(BF16)
                    x_all[1, rows, at : at + LANES] = (g_real * p_imag + g_imag * p_real).astype(BF16)
        return carry

    lax.fori_loop(0, classes, form, 0)

    order_in, order_out = iota((WIDE, WIDE), 0), iota((WIDE, WIDE), 1)
    wanted = order_out // dirs % BLOCK * LANES + order_out // (BLOCK * dirs) * dirs + order_out % dirs
    shuffle = ones_where(order_in == wanted)

    def finish(t, ext):
        lanes = pl.ds(pl.multiple_of(t * WIDE, WIDE), WIDE)
        z_real = dot(matrix[...], x_all[0, :, lanes])
        z_imag = dot(matrix[...], x_all[1, :, lanes])
        y_real = z_real[:modes] - z_imag[modes:]
        y_imag = z_real[modes:] + z_imag[:modes]
        m_real, m_imag = mie_wide[:modes, lanes], mie_wide[modes:, lanes]
        o_real = base[:modes, lanes] + (m_real * y_real - m_imag * y_imag)
        o_imag = base[modes:, lanes] + (m_real * y_imag + m_imag * y_real)
        term = inc[:modes, lanes] * o_real + inc[modes:, lanes] * o_imag
        out_ref[:modes, lanes] = dot(o_real.astype(BF16), shuffle).astype(BF16)
        out_ref[modes:, lanes] = dot(o_imag.astype(BF16), shuffle).astype(BF16)
        return ext + term.reshape(modes // 8, 8, WIDE).sum(0)

    ext = lax.fori_loop(0, tiles, finish, jnp.zeros((8, WIDE), F32))
    local = (ext[:, :LANES] + ext[:, LANES:]).sum(0, keepdims=True)
    ext_send[...] = local
    ext_recv[me] = local

    def ext_copy(i, landing):
        offset = offset_of(i)
        here = lax.rem(me + devices - offset, devices) if landing else me
        return exchange(ext_send, ext_recv.at[here], esend_sem, erecv_sem, offset)

    def start_ext(i, carry):
        ext_copy(i, False).start()
        return carry

    def end_ext(i, carry):
        copy = ext_copy(i, True)
        copy.wait_send()
        copy.wait_recv()
        return carry

    lax.fori_loop(0, devices - 1, start_ext, 0)
    lax.fori_loop(0, devices - 1, end_ext, 0)
    total = jnp.broadcast_to(ext_recv[...].sum(0), (8, LANES))
    shift = LANES // 2
    while shift >= dirs:
        total = total + pltpu.roll(total, shift, 1)
        shift //= 2
    ext_ref[...] = total[0:1, 0:dirs]


def shards(
    positions, wave_vectors, pattern, dir_index, mie, trans_table, pair_route, pair_source, pair_target, pair_class,
):
    modes = pattern.shape[1]
    spheres = positions.shape[0]
    dirs = dir_index.shape[0]
    devices = lax.axis_size("sph")
    groups = lax.axis_size("groups")
    pairs = pair_source.shape[0]
    classes = trans_table.shape[0]
    both = 2 * modes
    columns = spheres * dirs
    units = both // LANES + 1
    share = 4 * units // groups
    slots = 2 * devices
    vmem = pl.BlockSpec(memory_space=pltpu.VMEM)
    dma = pltpu.SemaphoreType.DMA
    scattered, extinction = pl.pallas_call(
        body,
        out_shape=(
            jax.ShapeDtypeStruct((both, columns), BF16),
            jax.ShapeDtypeStruct((1, dirs), F32),
        ),
        in_specs=[vmem] * 9 + [pl.BlockSpec(memory_space=pl.ANY)],
        out_specs=(vmem, vmem),
        scratch_shapes=[
            pltpu.VMEM((max(1, units // share), devices, share, LANES), BF16),
            pltpu.VMEM((groups, devices, share, LANES), BF16),
            pltpu.VMEM((1, LANES), F32),
            pltpu.VMEM((devices, 1, LANES), F32),
            pltpu.VMEM((classes, both, modes), BF16),
            dma,
            dma((devices,)),
            dma((devices,)),
            dma((groups,)),
            dma((groups,)),
            dma((devices,)),
            dma((devices,)),
            pltpu.VMEM((LANES, spheres), F32),
            pltpu.VMEM((LANES, -(-modes // LANES) * LANES), F32),
            pltpu.VMEM((both, LANES), F32),
            pltpu.VMEM((both, columns), F32),
            pltpu.VMEM((both, columns), F32),
            pltpu.VMEM((both, columns), F32),
            pltpu.VMEM((2, both, 2 * slots), BF16),
            pltpu.VMEM((2, 2 * slots, columns // 2), BF16),
            pltpu.VMEM((both, classes * modes), BF16),
            pltpu.VMEM((2, classes * modes, columns), BF16),
        ],
        compiler_params=pltpu.CompilerParams(
            vmem_limit_bytes=63 * 1024 * 1024, collective_id=0, has_side_effects=True
        ),
        name="cluster",
    )(
        pair_route.reshape(1, pairs),
        pair_source[None],
        pair_target[None],
        pair_class[None],
        positions.T,
        wave_vectors.T,
        dir_index[None],
        mie.transpose(0, 2, 1),
        pattern.reshape(both, -1),
        trans_table.reshape(classes, both, modes),
    )
    return (scattered, extinction[0])


def solution(mesh):
    placed = (
        P("sph", None),
        P(),
        P(),
        P("groups"),
        P(None, None, "sph"),
        P(),
        P("sph", None),
        P("sph"),
        P("sph"),
        P("sph"),
    )
    return jax.shard_map(
        shards,
        mesh=mesh,
        in_specs=placed,
        out_specs=(P(None, ("groups", "sph")), P("groups")),
        check_vma=False,
    )
```

```python
import jax
import jax.numpy as jnp
from jax import lax
from jax.experimental import pallas as pl
from jax.experimental.pallas import tpu as pltpu
from jax.sharding import PartitionSpec as P

BLOCK = 2
LANES = 128
WIDE = 256
PART = 8
TARGET_AT = 24
CLASS_AT = 25
F32 = jnp.float32
BF16 = jnp.bfloat16
HIGHEST = lax.Precision.HIGHEST
MESH = pl.DeviceIdType.MESH
NT = (((1,), (1,)), ((), ()))


def iota(shape, axis):
    return lax.broadcasted_iota(jnp.int32, shape, axis)


def ones_where(mask):
    return mask.astype(F32).astype(BF16)


def split3(x):
    hi = x.astype(BF16)
    rest = x - hi.astype(F32)
    mid = rest.astype(BF16)
    low = (rest - mid.astype(F32)).astype(BF16)
    return hi, mid, low


def dot(a, b, **kw):
    return jnp.dot(a, b, preferred_element_type=F32, **kw)


ROWS = 16


def paired(x):
    return x.reshape(x.shape[0] // (2 * ROWS), 2, ROWS, x.shape[1])


def halves(x):
    groups = paired(x)
    flat = (x.shape[0] // 2, x.shape[1])
    return groups[:, 0].reshape(flat), groups[:, 1].reshape(flat)


def body(
    route_hbm, source_hbm, target_hbm, class_hbm, pos_hbm, wave_hbm, dirs_hbm, mie_hbm, pattern_hbm, table_hbm,
    out_hbm, ext_ref,
    route_ref, source_ref, target_ref, class_ref, pos_ref, wave_ref, dirs_ref, mie_ref, pattern_ref, load_sem,
    out_ref, out_sem, z_buf,
    send, recv, ext_send, ext_recv, table, table_sem, send_sem, recv_sem, gsend_sem, grecv_sem, esend_sem, erecv_sem,
    parts, mie_rows, pat, mie_wide, inc, base, left, weights, matrix, x_all,
):
    me = lax.axis_index("sph")
    group = lax.axis_index("groups")
    devices = lax.axis_size("sph")
    groups = lax.axis_size("groups")
    pairs = route_ref.shape[1]
    spheres, modes = mie_ref.shape[1:]
    both = 2 * modes
    classes = table.shape[0]
    columns = out_ref.shape[1]
    dirs = dirs_ref.shape[1]
    blocks = spheres // BLOCK
    tile_blocks = LANES // dirs
    tiles = blocks // tile_blocks
    slots = 2 * devices
    units = both // LANES + 1
    share = recv.shape[2]
    whole = modes // LANES

    barrier = pltpu.get_barrier_semaphore()

    def offset_of(i):
        return devices // 2 + (i + 1) // 2 * (1 - 2 * lax.rem(i, 2))

    def greet(i, carry):
        to = lax.rem(me + offset_of(i), devices)
        pl.semaphore_signal(barrier, inc=1, device_id={"sph": to}, device_id_type=MESH)
        return carry

    def greet_group(i, carry):
        pl.semaphore_signal(barrier, inc=1, device_id={"groups": lax.rem(group + i, groups)}, device_id_type=MESH)
        return carry

    lax.fori_loop(0, devices - 1, greet, 0)
    lax.fori_loop(1, groups, greet_group, 0)
    given = (route_hbm, source_hbm, target_hbm, class_hbm, pos_hbm, mie_hbm, wave_hbm, dirs_hbm, pattern_hbm)
    taken = (route_ref, source_ref, target_ref, class_ref, pos_ref, mie_ref, wave_ref, dirs_ref, pattern_ref)
    loads = [pltpu.make_async_copy(a, b, load_sem.at[i]) for i, (a, b) in enumerate(zip(given, taken))]
    load_table = pltpu.make_async_copy(table_hbm, table, table_sem)
    for load in loads:
        load.start()
    load_table.start()
    for load in loads[:6]:
        load.wait()

    named = ones_where(route_ref[...] == iota((devices, pairs), 0))
    earlier = ones_where(iota((pairs, pairs), 0) < iota((pairs, pairs), 1))
    before = dot(named, earlier)
    parts[...] = jnp.zeros_like(parts)
    for i, part in enumerate(split3(pos_ref[...])):
        parts[i * PART : i * PART + 3, :] = part.astype(F32)
    row = iota((LANES, pairs), 0)
    pair_meta = jnp.where(
        row == TARGET_AT, target_ref[...] + 1, jnp.where(row == CLASS_AT, class_ref[...], 0)
    ).astype(F32).astype(BF16)
    mixed = jnp.concatenate([mie_ref[0, :, whole * LANES :], mie_ref[1, :, whole * LANES :]], 1)
    first_unit = group * share
    rows_of_share = max(1, share // units)
    for n in range(rows_of_share):
        kind = first_unit // units + n
        rank = (kind // 2).astype(F32)
        sphere = lax.rem(kind, 2)
        slot = jnp.where(before == rank, named.astype(F32), 0.0).astype(BF16)
        origin = ones_where(source_ref[...] * BLOCK + sphere == iota((spheres, pairs), 0))
        pick = lax.dot_general(slot, origin, NT, preferred_element_type=F32).astype(BF16)
        meta = lax.dot_general(slot, pair_meta, NT, preferred_element_type=F32)
        where = lax.dot_general(pick, parts[...].astype(BF16), NT, preferred_element_type=F32)
        for u in range(units):
            if u == units - 1:
                value = where + meta
            else:
                c, t = divmod(u, whole)
                rows = mixed if c == 2 else mie_ref[c, :, t * LANES : (t + 1) * LANES]
                value = dot(pick, rows.astype(BF16))
            at = n * units + u
            send[at // share, :, at % share, :] = value.astype(BF16)
    piece = lax.rem(first_unit, units) // share if share < units else 0

    pl.semaphore_wait(barrier, devices + groups - 2)

    def exchange(src, dst, sends, receives, offset):
        return pltpu.make_async_remote_copy(
            src_ref=src,
            dst_ref=dst,
            send_sem=sends.at[offset],
            recv_sem=receives.at[offset],
            device_id={"sph": lax.rem(me + offset, devices)},
            device_id_type=MESH,
        )

    def slot_copy(i):
        offset = offset_of(i)
        to = lax.rem(me + offset, devices)
        return exchange(send.at[piece, to], recv.at[group, i], send_sem, recv_sem, offset)

    def start_slot(i, carry):
        slot_copy(i).start()
        return carry

    lax.fori_loop(0, devices - 1, start_slot, 0)
    recv[group, devices - 1] = send[piece, me]
    for load in loads[6:]:
        load.wait()

    lane_dir = dirs_ref[...]
    lane_dirs = jnp.concatenate([lane_dir] * tile_blocks, 1)
    select = (iota((pattern_ref.shape[1], LANES), 0) == lane_dirs).astype(F32)
    pat[...] = dot(pattern_ref[...], select, precision=HIGHEST)
    waves = dot(wave_ref[...], select, precision=HIGHEST)
    kx, ky, kz = waves[0:1], waves[1:2], waves[2:3]
    wide = iota((LANES, columns), 1)
    sphere_of = ((wide // WIDE) * tile_blocks + wide // dirs % tile_blocks) * BLOCK + wide // LANES % BLOCK
    spread = ones_where(lax.rem(iota((LANES, columns), 0), spheres) == sphere_of)
    own = dot(pos_ref[...], spread[0:spheres].astype(F32), precision=HIGHEST)
    mie_rows[...] = jnp.zeros_like(mie_rows)
    for c in range(2):
        for i, part in enumerate(split3(mie_ref[c])):
            mie_rows[i * spheres : (i + 1) * spheres, 0:modes] = part.astype(F32)
        mie_wide[c * modes : (c + 1) * modes, :] = dot(mie_rows[...].T[:modes].astype(BF16), spread)
    for n in range(columns // LANES):
        lanes = slice(n * LANES, (n + 1) * LANES)
        phase = own[0:1, lanes] * kx + own[1:2, lanes] * ky + own[2:3, lanes] * kz
        cosine, sine = jnp.cos(phase), jnp.sin(phase)
        p_real, p_imag = pat[:modes, :], pat[modes:, :]
        i_real = cosine * p_real - sine * p_imag
        i_imag = cosine * p_imag + sine * p_real
        m_real, m_imag = mie_wide[:modes, lanes], mie_wide[modes:, lanes]
        inc[:modes, lanes] = i_real
        inc[modes:, lanes] = i_imag
        base[:modes, lanes] = m_real * i_real - m_imag * i_imag
        base[modes:, lanes] = m_real * i_imag + m_imag * i_real
    load_table.wait()
    for c in range(classes // 2):
        two = jnp.concatenate([table[2 * c], table[2 * c + 1]], 1)
        for k in range(2):
            part = two[k * modes : (k + 1) * modes].reshape(modes // ROWS, ROWS, both)
            matrix[:, k, :, c * both : (c + 1) * both] = part

    def end_slot(i, carry):
        copy = slot_copy(i)
        copy.wait_send()
        copy.wait_recv()
        return carry

    quarter = devices // 4

    def share_copy(q, i, landing):
        at = lax.rem(group + groups - i, groups) if landing else group
        rows = pl.ds(q * quarter, quarter)
        return pltpu.make_async_remote_copy(
            src_ref=recv.at[group, rows],
            dst_ref=recv.at[at, rows],
            send_sem=gsend_sem.at[q, i],
            recv_sem=grecv_sem.at[q, i],
            device_id={"groups": lax.rem(group + i, groups)},
            device_id_type=MESH,
        )

    def start_share(q, carry):
        lax.fori_loop(q * quarter, jnp.minimum((q + 1) * quarter, devices - 1), end_slot, 0)

        def start_one(i, carry):
            share_copy(q, i, False).start()
            return carry

        return lax.fori_loop(1, groups, start_one, carry)

    def end_share(q, carry):
        def end_one(i, carry):
            copy = share_copy(q, i, True)
            copy.wait_send()
            copy.wait_recv()
            return carry

        return lax.fori_loop(1, groups, end_one, carry)

    lax.fori_loop(0, 4, start_share, 0)
    lax.fori_loop(0, 4, end_share, 0)

    def arrived(s, u):
        both_ranks = []
        for r in range(2):
            at = (2 * r + s) * units + u
            both_ranks.append(recv[at // share, :, at % share, :].astype(F32))
        return jnp.concatenate(both_ranks, 0)

    phases = []
    for s in range(2):
        for u in range(units - 1):
            c, t = divmod(u, whole)
            block = arrived(s, u).T.astype(BF16)
            if c < 2:
                groups_of = block.reshape(LANES // ROWS, ROWS, slots)
                at = slice(t * LANES // ROWS, (t + 1) * LANES // ROWS)
                left[s, at, c, :, 0:slots] = groups_of
                left[s, at, 1 - c, :, slots : 2 * slots] = -groups_of if c else groups_of
            else:
                rest = modes - whole * LANES
                at = slice(whole * LANES // ROWS, modes // ROWS)
                for c in range(2):
                    groups_of = block[c * rest : (c + 1) * rest].reshape(rest // ROWS, ROWS, slots)
                    left[s, at, c, :, 0:slots] = groups_of
                    left[s, at, 1 - c, :, slots : 2 * slots] = -groups_of if c else groups_of
        meta = arrived(s, units - 1)
        x, y, z = (
            meta[:, i : i + 1] + meta[:, PART + i : PART + i + 1] + meta[:, 2 * PART + i : 2 * PART + i + 1]
            for i in range(3)
        )
        phase = x * kx + y * ky + z * kz
        phases.append((jnp.cos(phase), jnp.sin(phase)))
    target = meta[:, TARGET_AT : TARGET_AT + 1]
    code = jnp.where(target > 0.0, meta[:, CLASS_AT : CLASS_AT + 1] * float(blocks) + target - 1.0, -1.0)
    code = jnp.broadcast_to(code, (slots, LANES))

    def form(c, carry):
        rows = pl.ds(pl.multiple_of(c * modes, 64), modes)
        for s in range(2):
            cosine, sine = phases[s]
            for t in range(tiles):
                block_of = (iota((slots, LANES), 1) // dirs + t * tile_blocks + c * blocks).astype(F32)
                hit = code == block_of
                lanes = slice(t * LANES, (t + 1) * LANES)
                weights[s, 0:slots, lanes] = jnp.where(hit, cosine, 0.0).astype(BF16)
                weights[s, slots : 2 * slots, lanes] = jnp.where(hit, sine, 0.0).astype(BF16)
        for s in range(2):
            for n in range(tiles // 2):
                gathered = dot(left[s].reshape(both, 2 * slots), weights[s, :, n * WIDE : (n + 1) * WIDE])
                for t in range(2):
                    lanes = slice(t * LANES, (t + 1) * LANES)
                    g_real, g_imag = halves(gathered[:, lanes])
                    p_real, p_imag = pat[:modes, :], pat[modes:, :]
                    at = (2 * n + t) * WIDE + s * LANES
                    x_all[0, rows, at : at + LANES] = (g_real * p_real - g_imag * p_imag).astype(BF16)
                    x_all[1, rows, at : at + LANES] = (g_real * p_imag + g_imag * p_real).astype(BF16)
        return carry

    lax.fori_loop(0, classes, form, 0)

    def multiply(t):
        lanes = slice(t * WIDE, (t + 1) * WIDE)
        for k in range(2):
            z_buf[t % 2, k] = dot(matrix[...].reshape(both, classes * modes), x_all[k, :, lanes])

    def fold(t, ext):
        lanes = slice(t * WIDE, (t + 1) * WIDE)
        real_real, imag_real = halves(z_buf[t % 2, 0])
        real_imag, imag_imag = halves(z_buf[t % 2, 1])
        y_real = real_real - imag_imag
        y_imag = imag_real + real_imag
        m_real, m_imag = mie_wide[:modes, lanes], mie_wide[modes:, lanes]
        o_real = base[:modes, lanes] + (m_real * y_real - m_imag * y_imag)
        o_imag = base[modes:, lanes] + (m_real * y_imag + m_imag * y_real)
        out_ref[:modes, lanes] = o_real.astype(BF16)
        out_ref[modes:, lanes] = o_imag.astype(BF16)
        term = inc[:modes, lanes] * o_real + inc[modes:, lanes] * o_imag
        return ext + term.reshape(modes // 8, 8, WIDE).sum(0)

    ext = jnp.zeros((8, WIDE), F32)
    multiply(0)
    for t in range(1, tiles):
        multiply(t)
        ext = fold(t - 1, ext)
    ext = fold(tiles - 1, ext)
    local = (ext[:, :LANES] + ext[:, LANES:]).sum(0, keepdims=True)
    ext_send[...] = local
    ext_recv[me] = local

    def ext_copy(i, landing):
        offset = offset_of(i)
        here = lax.rem(me + devices - offset, devices) if landing else me
        return exchange(ext_send, ext_recv.at[here], esend_sem, erecv_sem, offset)

    def start_ext(i, carry):
        ext_copy(i, False).start()
        return carry

    def end_ext(i, carry):
        copy = ext_copy(i, True)
        copy.wait_send()
        copy.wait_recv()
        return carry

    lax.fori_loop(0, devices - 1, start_ext, 0)
    store = pltpu.make_async_copy(out_ref, out_hbm, out_sem)
    store.start()
    store.wait()
    lax.fori_loop(0, devices - 1, end_ext, 0)
    ext_ref[...] = ext_recv[...].sum(0)


def order_kernel(mixed_ref, lanes_ref, out_ref, ext_ref):
    dirs = ext_ref.shape[1]
    order_in, order_out = iota((WIDE, WIDE), 0), iota((WIDE, WIDE), 1)
    wanted = order_out // dirs % BLOCK * LANES + order_out // (BLOCK * dirs) * dirs + order_out % dirs
    shuffle = ones_where(order_in == wanted)
    out_ref[...] = dot(mixed_ref[...], shuffle).astype(BF16)
    total = jnp.broadcast_to(lanes_ref[...], (8, LANES))
    shift = LANES // 2
    while shift >= dirs:
        total = total + pltpu.roll(total, shift, 1)
        shift //= 2
    ext_ref[...] = total[0:1, 0:dirs]


def shards(
    positions, wave_vectors, pattern, dir_index, mie, trans_table, pair_route, pair_source, pair_target, pair_class,
):
    modes = pattern.shape[1]
    spheres = positions.shape[0]
    dirs = dir_index.shape[0]
    devices = lax.axis_size("sph")
    groups = lax.axis_size("groups")
    pairs = pair_source.shape[0]
    classes = trans_table.shape[0]
    both = 2 * modes
    columns = spheres * dirs
    units = both // LANES + 1
    share = 4 * units // groups
    slots = 2 * devices
    vmem = pl.BlockSpec(memory_space=pltpu.VMEM)
    anywhere = pl.BlockSpec(memory_space=pl.ANY)
    dma = pltpu.SemaphoreType.DMA
    mixed, lane_sums = pl.pallas_call(
        body,
        out_shape=(
            jax.ShapeDtypeStruct((both, columns), BF16),
            jax.ShapeDtypeStruct((1, LANES), F32),
        ),
        in_specs=[anywhere] * 10,
        out_specs=(anywhere, vmem),
        scratch_shapes=[
            *[pltpu.VMEM((1, pairs), jnp.int32)] * 4,
            pltpu.VMEM((3, spheres), F32),
            pltpu.VMEM((3, wave_vectors.shape[0]), F32),
            pltpu.VMEM((1, dirs), jnp.int32),
            pltpu.VMEM((2, spheres, modes), F32),
            pltpu.VMEM((both, wave_vectors.shape[0]), F32),
            dma((9,)),
            pltpu.VMEM((both, columns), BF16),
            dma,
            pltpu.VMEM((2, 2, both, WIDE), F32),
            pltpu.VMEM((max(1, units // share), devices, share, LANES), BF16),
            pltpu.VMEM((groups, devices, share, LANES), BF16),
            pltpu.VMEM((1, LANES), F32),
            pltpu.VMEM((devices, 1, LANES), F32),
            pltpu.VMEM((classes, both, modes), BF16),
            dma,
            dma((devices,)),
            dma((devices,)),
            dma((4, groups)),
            dma((4, groups)),
            dma((devices,)),
            dma((devices,)),
            pltpu.VMEM((LANES, spheres), F32),
            pltpu.VMEM((LANES, -(-modes // LANES) * LANES), F32),
            pltpu.VMEM((both, LANES), F32),
            pltpu.VMEM((both, columns), F32),
            pltpu.VMEM((both, columns), F32),
            pltpu.VMEM((both, columns), F32),
            pltpu.VMEM((2, modes // ROWS, 2, ROWS, 2 * slots), BF16),
            pltpu.VMEM((2, 2 * slots, columns // 2), BF16),
            pltpu.VMEM((modes // ROWS, 2, ROWS, classes * modes), BF16),
            pltpu.VMEM((2, classes * modes, columns), BF16),
        ],
        compiler_params=pltpu.CompilerParams(
            vmem_limit_bytes=63 * 1024 * 1024, collective_id=0, has_side_effects=True
        ),
        name="cluster",
    )(
        pair_route.reshape(1, pairs),
        pair_source[None],
        pair_target[None],
        pair_class[None],
        positions.T,
        wave_vectors.T,
        dir_index[None],
        mie.transpose(0, 2, 1),
        pattern.reshape(both, -1),
        trans_table.reshape(classes, both, modes),
    )
    block = pl.BlockSpec((both, WIDE), lambda t: (0, t))
    scattered, extinction = pl.pallas_call(
        order_kernel,
        out_shape=(
            jax.ShapeDtypeStruct((both, columns), BF16),
            jax.ShapeDtypeStruct((1, dirs), F32),
        ),
        grid=(columns // WIDE,),
        in_specs=[block, pl.BlockSpec((1, LANES), lambda t: (0, 0))],
        out_specs=(block, pl.BlockSpec((1, dirs), lambda t: (0, 0))),
        name="order",
    )(mixed, lane_sums)
    return (scattered, extinction[0])


def solution(mesh):
    placed = (
        P("sph", None),
        P(),
        P(),
        P("groups"),
        P(None, None, "sph"),
        P(),
        P("sph", None),
        P("sph"),
        P("sph"),
        P("sph"),
    )
    return jax.shard_map(
        shards,
        mesh=mesh,
        in_specs=placed,
        out_specs=(P(None, ("groups", "sph")), P("groups")),
        check_vma=False,
    )
```

```python
import jax
import jax.numpy as jnp
from jax import lax
from jax.experimental import pallas as pl
from jax.experimental.pallas import tpu as pltpu
from jax.sharding import PartitionSpec as P

BLOCK = 2
LANES = 128
WIDE = 256
PART = 8
TARGET_AT = 24
CLASS_AT = 25
F32 = jnp.float32
BF16 = jnp.bfloat16
HIGHEST = lax.Precision.HIGHEST
MESH = pl.DeviceIdType.MESH
NT = (((1,), (1,)), ((), ()))


def iota(shape, axis):
    return lax.broadcasted_iota(jnp.int32, shape, axis)


def ones_where(mask):
    return mask.astype(F32).astype(BF16)


def split3(x):
    hi = x.astype(BF16)
    rest = x - hi.astype(F32)
    mid = rest.astype(BF16)
    low = (rest - mid.astype(F32)).astype(BF16)
    return hi, mid, low


def dot(a, b, **kw):
    return jnp.dot(a, b, preferred_element_type=F32, **kw)


ROWS = 16


def paired(x):
    return x.reshape(x.shape[0] // (2 * ROWS), 2, ROWS, x.shape[1])


def halves(x):
    groups = paired(x)
    flat = (x.shape[0] // 2, x.shape[1])
    return groups[:, 0].reshape(flat), groups[:, 1].reshape(flat)


def body(
    route_hbm, source_hbm, target_hbm, class_hbm, pos_hbm, wave_hbm, dirs_hbm, mie_hbm, pattern_hbm, table_hbm,
    out_hbm, ext_ref,
    route_ref, source_ref, target_ref, class_ref, pos_ref, wave_ref, dirs_ref, mie_ref, pattern_ref, load_sem,
    out_ref, ordered, out_sem, z_buf,
    send, recv, ext_send, ext_recv, table, table_sem, send_sem, recv_sem, gsend_sem, grecv_sem, esend_sem, erecv_sem,
    parts, mie_rows, pat, mie_wide, inc, base, left, weights, matrix, x_all,
):
    me = lax.axis_index("sph")
    group = lax.axis_index("groups")
    devices = lax.axis_size("sph")
    groups = lax.axis_size("groups")
    pairs = route_ref.shape[1]
    spheres, modes = mie_ref.shape[1:]
    both = 2 * modes
    classes = table.shape[0]
    columns = out_ref.shape[1]
    dirs = dirs_ref.shape[1]
    blocks = spheres // BLOCK
    tile_blocks = LANES // dirs
    tiles = blocks // tile_blocks
    slots = 2 * devices
    units = both // LANES + 1
    share = recv.shape[2]
    whole = modes // LANES

    barrier = pltpu.get_barrier_semaphore()

    middle = devices // 2
    stride = 5

    def each_peer(act):
        def pair(e):
            for number, offset in ((2 * e, middle - e), (2 * e + 1, middle + 1 + e)):
                to = me + offset
                act(number, jnp.where(to >= devices, to - devices, to))

        def some(j, carry):
            for u in range(stride):
                pair(j * stride + u)
            return carry

        lax.fori_loop(0, (middle - 1) // stride, some, 0)
        for e in range((middle - 1) // stride * stride, middle - 1):
            pair(e)
        to = me + 1
        act(devices - 2, jnp.where(to >= devices, to - devices, to))

    def greet(number, to):
        pl.semaphore_signal(barrier, inc=1, device_id={"sph": to}, device_id_type=MESH)

    def greet_group(i, carry):
        pl.semaphore_signal(barrier, inc=1, device_id={"groups": lax.rem(group + i, groups)}, device_id_type=MESH)
        return carry

    each_peer(greet)
    lax.fori_loop(1, groups, greet_group, 0)
    given = (route_hbm, source_hbm, target_hbm, class_hbm, pos_hbm, mie_hbm, wave_hbm, dirs_hbm, pattern_hbm)
    taken = (route_ref, source_ref, target_ref, class_ref, pos_ref, mie_ref, wave_ref, dirs_ref, pattern_ref)
    loads = [pltpu.make_async_copy(a, b, load_sem.at[i]) for i, (a, b) in enumerate(zip(given, taken))]
    load_table = pltpu.make_async_copy(table_hbm, table, table_sem)
    for load in loads:
        load.start()
    load_table.start()
    for load in loads[:6]:
        load.wait()

    named = ones_where(route_ref[...] == iota((devices, pairs), 0))
    earlier = ones_where(iota((pairs, pairs), 0) < iota((pairs, pairs), 1))
    before = dot(named, earlier)
    parts[...] = jnp.zeros_like(parts)
    for i, part in enumerate(split3(pos_ref[...])):
        parts[i * PART : i * PART + 3, :] = part.astype(F32)
    row = iota((LANES, pairs), 0)
    pair_meta = jnp.where(
        row == TARGET_AT, target_ref[...] + 1, jnp.where(row == CLASS_AT, class_ref[...], 0)
    ).astype(F32).astype(BF16)
    mixed = jnp.concatenate([mie_ref[0, :, whole * LANES :], mie_ref[1, :, whole * LANES :]], 1)
    first_unit = group * share
    rows_of_share = max(1, share // units)
    for n in range(rows_of_share):
        kind = first_unit // units + n
        rank = (kind // 2).astype(F32)
        sphere = lax.rem(kind, 2)
        slot = jnp.where(before == rank, named.astype(F32), 0.0).astype(BF16)
        origin = ones_where(source_ref[...] * BLOCK + sphere == iota((spheres, pairs), 0))
        pick = lax.dot_general(slot, origin, NT, preferred_element_type=F32).astype(BF16)
        meta = lax.dot_general(slot, pair_meta, NT, preferred_element_type=F32)
        where = lax.dot_general(pick, parts[...].astype(BF16), NT, preferred_element_type=F32)
        for u in range(units):
            if u == units - 1:
                value = where + meta
            else:
                c, t = divmod(u, whole)
                rows = mixed if c == 2 else mie_ref[c, :, t * LANES : (t + 1) * LANES]
                value = dot(pick, rows.astype(BF16))
            at = n * units + u
            send[at // share, :, at % share, :] = value.astype(BF16)
    piece = lax.rem(first_unit, units) // share if share < units else 0

    pl.semaphore_wait(barrier, devices + groups - 2)

    def exchange(src, dst, sends, receives, number, to):
        return pltpu.make_async_remote_copy(
            src_ref=src,
            dst_ref=dst,
            send_sem=sends.at[number],
            recv_sem=receives.at[number],
            device_id={"sph": to},
            device_id_type=MESH,
        )

    neighbour = jnp.where(me + 1 >= devices, 0, me + 1)

    def slot_copy(number, to):
        return exchange(send.at[piece, to], recv.at[group, number], send_sem, recv_sem, number, to)

    each_peer(lambda number, to: slot_copy(number, to).start())
    recv[group, devices - 1] = send[piece, me]
    for load in loads[6:]:
        load.wait()

    lane_dir = dirs_ref[...]
    lane_dirs = jnp.concatenate([lane_dir] * tile_blocks, 1)
    select = (iota((pattern_ref.shape[1], LANES), 0) == lane_dirs).astype(F32)
    pat[...] = dot(pattern_ref[...], select, precision=HIGHEST)
    waves = dot(wave_ref[...], select, precision=HIGHEST)
    kx, ky, kz = waves[0:1], waves[1:2], waves[2:3]
    wide = iota((LANES, columns), 1)
    sphere_of = ((wide // WIDE) * tile_blocks + wide // dirs % tile_blocks) * BLOCK + wide // LANES % BLOCK
    spread = ones_where(lax.rem(iota((LANES, columns), 0), spheres) == sphere_of)
    own = dot(pos_ref[...], spread[0:spheres].astype(F32), precision=HIGHEST)
    mie_rows[...] = jnp.zeros_like(mie_rows)
    for c in range(2):
        for i, part in enumerate(split3(mie_ref[c])):
            mie_rows[i * spheres : (i + 1) * spheres, 0:modes] = part.astype(F32)
        mie_wide[c * modes : (c + 1) * modes, :] = dot(mie_rows[...].T[:modes].astype(BF16), spread)
    for n in range(columns // LANES):
        lanes = slice(n * LANES, (n + 1) * LANES)
        phase = own[0:1, lanes] * kx + own[1:2, lanes] * ky + own[2:3, lanes] * kz
        cosine, sine = jnp.cos(phase), jnp.sin(phase)
        p_real, p_imag = pat[:modes, :], pat[modes:, :]
        i_real = cosine * p_real - sine * p_imag
        i_imag = cosine * p_imag + sine * p_real
        m_real, m_imag = mie_wide[:modes, lanes], mie_wide[modes:, lanes]
        inc[:modes, lanes] = i_real
        inc[modes:, lanes] = i_imag
        base[:modes, lanes] = m_real * i_real - m_imag * i_imag
        base[modes:, lanes] = m_real * i_imag + m_imag * i_real
    load_table.wait()
    for c in range(classes // 2):
        two = jnp.concatenate([table[2 * c], table[2 * c + 1]], 1)
        for k in range(2):
            part = two[k * modes : (k + 1) * modes].reshape(modes // ROWS, ROWS, both)
            matrix[:, k, :, c * both : (c + 1) * both] = part

    def end_slot(i, carry):
        copy = slot_copy(i, neighbour)
        copy.wait_send()
        copy.wait_recv()
        return carry

    quarter = devices // 4

    def share_copy(q, i, landing):
        at = lax.rem(group + groups - i, groups) if landing else group
        rows = pl.ds(q * quarter, quarter)
        return pltpu.make_async_remote_copy(
            src_ref=recv.at[group, rows],
            dst_ref=recv.at[at, rows],
            send_sem=gsend_sem.at[q, i],
            recv_sem=grecv_sem.at[q, i],
            device_id={"groups": lax.rem(group + i, groups)},
            device_id_type=MESH,
        )

    def start_share(q):
        lax.fori_loop(q * quarter, min((q + 1) * quarter, devices - 1), end_slot, 0)

        def start_one(i, carry):
            share_copy(q, i, False).start()
            return carry

        lax.fori_loop(1, groups, start_one, 0)

    def end_share(q, carry):
        def end_one(i, carry):
            copy = share_copy(q, i, True)
            copy.wait_send()
            copy.wait_recv()
            return carry

        return lax.fori_loop(1, groups, end_one, carry)

    for q in (3, 0, 2, 1):
        start_share(q)
    lax.fori_loop(0, 4, end_share, 0)

    def arrived(s, u):
        both_ranks = []
        for r in range(2):
            at = (2 * r + s) * units + u
            both_ranks.append(recv[at // share, :, at % share, :].astype(F32))
        return jnp.concatenate(both_ranks, 0)

    phases = []
    for s in range(2):
        for u in range(units - 1):
            c, t = divmod(u, whole)
            block = arrived(s, u).T.astype(BF16)
            if c < 2:
                groups_of = block.reshape(LANES // ROWS, ROWS, slots)
                at = slice(t * LANES // ROWS, (t + 1) * LANES // ROWS)
                left[s, at, c, :, 0:slots] = groups_of
                left[s, at, 1 - c, :, slots : 2 * slots] = -groups_of if c else groups_of
            else:
                rest = modes - whole * LANES
                at = slice(whole * LANES // ROWS, modes // ROWS)
                for c in range(2):
                    groups_of = block[c * rest : (c + 1) * rest].reshape(rest // ROWS, ROWS, slots)
                    left[s, at, c, :, 0:slots] = groups_of
                    left[s, at, 1 - c, :, slots : 2 * slots] = -groups_of if c else groups_of
        meta = arrived(s, units - 1)
        x, y, z = (
            meta[:, i : i + 1] + meta[:, PART + i : PART + i + 1] + meta[:, 2 * PART + i : 2 * PART + i + 1]
            for i in range(3)
        )
        phase = x * kx + y * ky + z * kz
        phases.append((jnp.cos(phase), jnp.sin(phase)))
    target = meta[:, TARGET_AT : TARGET_AT + 1]
    code = jnp.where(target > 0.0, meta[:, CLASS_AT : CLASS_AT + 1] * float(blocks) + target - 1.0, -1.0)
    code = jnp.broadcast_to(code, (slots, LANES))

    def form(c, carry):
        rows = pl.ds(pl.multiple_of(c * modes, 64), modes)
        for s in range(2):
            cosine, sine = phases[s]
            for t in range(tiles):
                block_of = (iota((slots, LANES), 1) // dirs + t * tile_blocks + c * blocks).astype(F32)
                hit = code == block_of
                lanes = slice(t * LANES, (t + 1) * LANES)
                weights[s, 0:slots, lanes] = jnp.where(hit, cosine, 0.0).astype(BF16)
                weights[s, slots : 2 * slots, lanes] = jnp.where(hit, sine, 0.0).astype(BF16)
        for s in range(2):
            for n in range(tiles // 2):
                gathered = dot(left[s].reshape(both, 2 * slots), weights[s, :, n * WIDE : (n + 1) * WIDE])
                for t in range(2):
                    lanes = slice(t * LANES, (t + 1) * LANES)
                    g_real, g_imag = halves(gathered[:, lanes])
                    p_real, p_imag = pat[:modes, :], pat[modes:, :]
                    at = (2 * n + t) * WIDE + s * LANES
                    x_all[0, rows, at : at + LANES] = (g_real * p_real - g_imag * p_imag).astype(BF16)
                    x_all[1, rows, at : at + LANES] = (g_real * p_imag + g_imag * p_real).astype(BF16)
        return carry

    lax.fori_loop(0, classes, form, 0)

    def multiply(t):
        lanes = slice(t * WIDE, (t + 1) * WIDE)
        for k in range(2):
            z_buf[t % 2, k] = dot(matrix[...].reshape(both, classes * modes), x_all[k, :, lanes])

    def fold(t, ext):
        lanes = slice(t * WIDE, (t + 1) * WIDE)
        real_real, imag_real = halves(z_buf[t % 2, 0])
        real_imag, imag_imag = halves(z_buf[t % 2, 1])
        y_real = real_real - imag_imag
        y_imag = imag_real + real_imag
        m_real, m_imag = mie_wide[:modes, lanes], mie_wide[modes:, lanes]
        o_real = base[:modes, lanes] + (m_real * y_real - m_imag * y_imag)
        o_imag = base[modes:, lanes] + (m_real * y_imag + m_imag * y_real)
        out_ref[:modes, lanes] = o_real.astype(BF16)
        out_ref[modes:, lanes] = o_imag.astype(BF16)
        term = inc[:modes, lanes] * o_real + inc[modes:, lanes] * o_imag
        return ext + term.reshape(modes // 8, 8, WIDE).sum(0)

    ext = jnp.zeros((8, WIDE), F32)
    multiply(0)
    for t in range(1, tiles):
        multiply(t)
        ext = fold(t - 1, ext)
    ext = fold(tiles - 1, ext)
    local = (ext[:, :LANES] + ext[:, LANES:]).sum(0, keepdims=True)
    ext_send[...] = local
    ext_recv[devices - 1] = local

    def ext_copy(number, to, here):
        return exchange(ext_send, ext_recv.at[here], esend_sem, erecv_sem, number, to)

    each_peer(lambda number, to: ext_copy(number, to, number).start())

    order_in, order_out = iota((WIDE, WIDE), 0), iota((WIDE, WIDE), 1)
    wanted = order_out // dirs % BLOCK * LANES + order_out // (BLOCK * dirs) * dirs + order_out % dirs
    shuffle = ones_where(order_in == wanted)
    stores = []
    for t in range(tiles):
        lanes = slice(t * WIDE, (t + 1) * WIDE)
        ordered[t] = dot(out_ref[:, lanes], shuffle).astype(BF16)
    for t in range(tiles):
        lanes = slice(t * WIDE, (t + 1) * WIDE)
        stores.append(pltpu.make_async_copy(ordered.at[t], out_hbm.at[:, lanes], out_sem.at[t]))
        stores[-1].start()
    for store in stores:
        store.wait()

    def end_ext(i, carry):
        copy = ext_copy(i, neighbour, i)
        copy.wait_send()
        copy.wait_recv()
        return carry

    lax.fori_loop(0, devices - 1, end_ext, 0)
    total = jnp.broadcast_to(ext_recv[...].sum(0), (8, LANES))
    shift = LANES // 2
    while shift >= dirs:
        total = total + pltpu.roll(total, shift, 1)
        shift //= 2
    ext_ref[...] = total[0:1]


def hand_over(from_hbm, sums_ref, to_hbm, ext_ref, held, in_sem, out_sem):
    count = held.shape[0]
    rows = held.shape[1]
    takes, gives = [], []
    for i in range(count):
        at = slice(i * rows, (i + 1) * rows)
        takes.append(pltpu.make_async_copy(from_hbm.at[at], held.at[i], in_sem.at[i]))
        gives.append(pltpu.make_async_copy(held.at[i], to_hbm.at[at], out_sem.at[i]))
        takes[i].start()
    ext_ref[...] = sums_ref[0:1, 0 : ext_ref.shape[1]]
    for i in range(count):
        takes[i].wait()
        gives[i].start()
    for i in range(count):
        gives[i].wait()


def shards(
    positions, wave_vectors, pattern, dir_index, mie, trans_table, pair_route, pair_source, pair_target, pair_class,
):
    modes = pattern.shape[1]
    spheres = positions.shape[0]
    dirs = dir_index.shape[0]
    devices = lax.axis_size("sph")
    groups = lax.axis_size("groups")
    pairs = pair_source.shape[0]
    classes = trans_table.shape[0]
    both = 2 * modes
    columns = spheres * dirs
    units = both // LANES + 1
    share = 4 * units // groups
    slots = 2 * devices
    vmem = pl.BlockSpec(memory_space=pltpu.VMEM)
    anywhere = pl.BlockSpec(memory_space=pl.ANY)
    dma = pltpu.SemaphoreType.DMA
    mixed, lane_sums = pl.pallas_call(
        body,
        out_shape=(
            jax.ShapeDtypeStruct((both, columns), BF16),
            jax.ShapeDtypeStruct((1, LANES), F32),
        ),
        in_specs=[anywhere] * 10,
        out_specs=(anywhere, vmem),
        scratch_shapes=[
            *[pltpu.VMEM((1, pairs), jnp.int32)] * 4,
            pltpu.VMEM((3, spheres), F32),
            pltpu.VMEM((3, wave_vectors.shape[0]), F32),
            pltpu.VMEM((1, dirs), jnp.int32),
            pltpu.VMEM((2, spheres, modes), F32),
            pltpu.VMEM((both, wave_vectors.shape[0]), F32),
            dma((9,)),
            pltpu.VMEM((both, columns), BF16),
            pltpu.VMEM((columns // WIDE, both, WIDE), BF16),
            dma((columns // WIDE,)),
            pltpu.VMEM((2, 2, both, WIDE), F32),
            pltpu.VMEM((max(1, units // share), devices, share, LANES), BF16),
            pltpu.VMEM((groups, devices, share, LANES), BF16),
            pltpu.VMEM((1, LANES), F32),
            pltpu.VMEM((devices, 1, LANES), F32),
            pltpu.VMEM((classes, both, modes), BF16),
            dma,
            dma((devices,)),
            dma((devices,)),
            dma((4, groups)),
            dma((4, groups)),
            dma((devices,)),
            dma((devices,)),
            pltpu.VMEM((LANES, spheres), F32),
            pltpu.VMEM((LANES, -(-modes // LANES) * LANES), F32),
            pltpu.VMEM((both, LANES), F32),
            pltpu.VMEM((both, columns), F32),
            pltpu.VMEM((both, columns), F32),
            pltpu.VMEM((both, columns), F32),
            pltpu.VMEM((2, modes // ROWS, 2, ROWS, 2 * slots), BF16),
            pltpu.VMEM((2, 2 * slots, columns // 2), BF16),
            pltpu.VMEM((modes // ROWS, 2, ROWS, classes * modes), BF16),
            pltpu.VMEM((2, classes * modes, columns), BF16),
        ],
        compiler_params=pltpu.CompilerParams(
            vmem_limit_bytes=63 * 1024 * 1024, collective_id=0, has_side_effects=True
        ),
        name="cluster",
    )(
        pair_route.reshape(1, pairs),
        pair_source[None],
        pair_target[None],
        pair_class[None],
        positions.T,
        wave_vectors.T,
        dir_index[None],
        mie.transpose(0, 2, 1),
        pattern.reshape(both, -1),
        trans_table.reshape(classes, both, modes),
    )
    pieces = 8
    scattered, extinction = pl.pallas_call(
        hand_over,
        out_shape=(
            jax.ShapeDtypeStruct((both, columns), BF16),
            jax.ShapeDtypeStruct((1, dirs), F32),
        ),
        in_specs=[anywhere, vmem],
        out_specs=(anywhere, vmem),
        scratch_shapes=[
            pltpu.VMEM((pieces, both // pieces, columns), BF16),
            dma((pieces,)),
            dma((pieces,)),
        ],
        compiler_params=pltpu.CompilerParams(vmem_limit_bytes=63 * 1024 * 1024),
        name="hand_over",
    )(mixed, lane_sums)
    return (scattered, extinction[0])


def solution(mesh):
    placed = (
        P("sph", None),
        P(),
        P(),
        P("groups"),
        P(None, None, "sph"),
        P(),
        P("sph", None),
        P("sph"),
        P("sph"),
        P("sph"),
    )
    return jax.shard_map(
        shards,
        mesh=mesh,
        in_specs=placed,
        out_specs=(P(None, ("groups", "sph")), P("groups")),
        check_vma=False,
    )
```

```python
import jax
import jax.numpy as jnp
from jax import lax
from jax.experimental import pallas as pl
from jax.experimental.pallas import tpu as pltpu
from jax.sharding import PartitionSpec as P

BLOCK = 2
LANES = 128
WIDE = 256
PART = 8
TARGET_AT = 24
CLASS_AT = 25
F32 = jnp.float32
BF16 = jnp.bfloat16
HIGHEST = lax.Precision.HIGHEST
MESH = pl.DeviceIdType.MESH
NT = (((1,), (1,)), ((), ()))


def iota(shape, axis):
    return lax.broadcasted_iota(jnp.int32, shape, axis)


def ones_where(mask):
    return mask.astype(F32).astype(BF16)


def split3(x):
    hi = x.astype(BF16)
    rest = x - hi.astype(F32)
    mid = rest.astype(BF16)
    low = (rest - mid.astype(F32)).astype(BF16)
    return hi, mid, low


def dot(a, b, **kw):
    return jnp.dot(a, b, preferred_element_type=F32, **kw)


ROWS = 16


def paired(x):
    return x.reshape(x.shape[0] // (2 * ROWS), 2, ROWS, x.shape[1])


def halves(x):
    groups = paired(x)
    flat = (x.shape[0] // 2, x.shape[1])
    return groups[:, 0].reshape(flat), groups[:, 1].reshape(flat)


def body(
    route_hbm, source_hbm, target_hbm, class_hbm, pos_hbm, wave_hbm, dirs_hbm, mie_hbm, pattern_hbm, table_hbm,
    out_hbm, ext_ref,
    route_ref, source_ref, target_ref, class_ref, pos_ref, wave_ref, dirs_ref, mie_ref, pattern_ref, load_sem,
    out_ref, ordered, out_sem, z_buf,
    send, recv, ext_send, ext_recv, table, table_sem, send_sem, recv_sem, gsend_sem, grecv_sem, esend_sem, erecv_sem,
    parts, mie_rows, pat, mie_wide, inc, base, left, weights, matrix, x_all,
):
    me = lax.axis_index("sph")
    group = lax.axis_index("groups")
    devices = lax.axis_size("sph")
    groups = lax.axis_size("groups")
    pairs = route_ref.shape[1]
    spheres, modes = mie_ref.shape[1:]
    both = 2 * modes
    classes = table.shape[0]
    columns = out_ref.shape[1]
    dirs = dirs_ref.shape[1]
    blocks = spheres // BLOCK
    tile_blocks = LANES // dirs
    tiles = blocks // tile_blocks
    slots = 2 * devices
    units = both // LANES + 1
    halvings, bit = recv.shape[0], recv.shape[3]
    share = halvings * bit
    whole = modes // LANES

    barrier = pltpu.get_barrier_semaphore()

    middle = devices // 2
    stride = 5

    def each_peer(act):
        def pair(e):
            for number, offset in ((2 * e, middle - e), (2 * e + 1, middle + 1 + e)):
                to = me + offset
                act(number, jnp.where(to >= devices, to - devices, to))

        def some(j, carry):
            for u in range(stride):
                pair(j * stride + u)
            return carry

        lax.fori_loop(0, (middle - 1) // stride, some, 0)
        for e in range((middle - 1) // stride * stride, middle - 1):
            pair(e)
        to = me + 1
        act(devices - 2, jnp.where(to >= devices, to - devices, to))

    def greet(number, to):
        pl.semaphore_signal(barrier, inc=1, device_id={"sph": to}, device_id_type=MESH)

    def greet_group(i, carry):
        pl.semaphore_signal(barrier, inc=1, device_id={"groups": lax.rem(group + i, groups)}, device_id_type=MESH)
        return carry

    each_peer(greet)
    lax.fori_loop(1, groups, greet_group, 0)
    given = (route_hbm, source_hbm, target_hbm, class_hbm, pos_hbm, mie_hbm, wave_hbm, dirs_hbm, pattern_hbm)
    taken = (route_ref, source_ref, target_ref, class_ref, pos_ref, mie_ref, wave_ref, dirs_ref, pattern_ref)
    loads = [pltpu.make_async_copy(a, b, load_sem.at[i]) for i, (a, b) in enumerate(zip(given, taken))]
    load_table = pltpu.make_async_copy(table_hbm, table, table_sem)
    for load in loads:
        load.start()
    load_table.start()
    for load in loads[:6]:
        load.wait()

    named = ones_where(route_ref[...] == iota((devices, pairs), 0))
    earlier = ones_where(iota((pairs, pairs), 0) < iota((pairs, pairs), 1))
    before = dot(named, earlier)
    parts[...] = jnp.zeros_like(parts)
    for i, part in enumerate(split3(pos_ref[...])):
        parts[i * PART : i * PART + 3, :] = part.astype(F32)
    row = iota((LANES, pairs), 0)
    pair_meta = jnp.where(
        row == TARGET_AT, target_ref[...] + 1, jnp.where(row == CLASS_AT, class_ref[...], 0)
    ).astype(F32).astype(BF16)
    mixed = jnp.concatenate([mie_ref[0, :, whole * LANES :], mie_ref[1, :, whole * LANES :]], 1)
    first_unit = group * share
    rows_of_share = max(1, share // units)
    for n in range(rows_of_share):
        kind = first_unit // units + n
        rank = (kind // 2).astype(F32)
        sphere = lax.rem(kind, 2)
        slot = jnp.where(before == rank, named.astype(F32), 0.0).astype(BF16)
        origin = ones_where(source_ref[...] * BLOCK + sphere == iota((spheres, pairs), 0))
        pick = lax.dot_general(slot, origin, NT, preferred_element_type=F32).astype(BF16)
        meta = lax.dot_general(slot, pair_meta, NT, preferred_element_type=F32)
        where = lax.dot_general(pick, parts[...].astype(BF16), NT, preferred_element_type=F32)
        for u in range(units):
            if u == units - 1:
                value = where + meta
            else:
                c, t = divmod(u, whole)
                rows = mixed if c == 2 else mie_ref[c, :, t * LANES : (t + 1) * LANES]
                value = dot(pick, rows.astype(BF16))
            at = n * units + u
            send[at % share // bit, at // share, :, at % bit, :] = value.astype(BF16)
    piece = lax.rem(first_unit, units) // share if share < units else 0

    pl.semaphore_wait(barrier, devices + groups - 2)

    def exchange(src, dst, sends, receives, number, to):
        return pltpu.make_async_remote_copy(
            src_ref=src,
            dst_ref=dst,
            send_sem=sends.at[number],
            recv_sem=receives.at[number],
            device_id={"sph": to},
            device_id_type=MESH,
        )

    neighbour = jnp.where(me + 1 >= devices, 0, me + 1)

    def slot_copy(h, number, to):
        return exchange(send.at[h, piece, to], recv.at[h, group, number], send_sem.at[h], recv_sem.at[h], number, to)

    for h in range(halvings):
        each_peer(lambda number, to: slot_copy(h, number, to).start())
        recv[h, group, devices - 1] = send[h, piece, me]
    for load in loads[6:]:
        load.wait()

    lane_dir = dirs_ref[...]
    lane_dirs = jnp.concatenate([lane_dir] * tile_blocks, 1)
    select = (iota((pattern_ref.shape[1], LANES), 0) == lane_dirs).astype(F32)
    pat[...] = dot(pattern_ref[...], select, precision=HIGHEST)
    waves = dot(wave_ref[...], select, precision=HIGHEST)
    kx, ky, kz = waves[0:1], waves[1:2], waves[2:3]
    wide = iota((LANES, columns), 1)
    sphere_of = ((wide // WIDE) * tile_blocks + wide // dirs % tile_blocks) * BLOCK + wide // LANES % BLOCK
    spread = ones_where(lax.rem(iota((LANES, columns), 0), spheres) == sphere_of)
    own = dot(pos_ref[...], spread[0:spheres].astype(F32), precision=HIGHEST)
    mie_rows[...] = jnp.zeros_like(mie_rows)
    for c in range(2):
        for i, part in enumerate(split3(mie_ref[c])):
            mie_rows[i * spheres : (i + 1) * spheres, 0:modes] = part.astype(F32)
        mie_wide[c * modes : (c + 1) * modes, :] = dot(mie_rows[...].T[:modes].astype(BF16), spread)
    for n in range(columns // LANES):
        lanes = slice(n * LANES, (n + 1) * LANES)
        phase = own[0:1, lanes] * kx + own[1:2, lanes] * ky + own[2:3, lanes] * kz
        cosine, sine = jnp.cos(phase), jnp.sin(phase)
        p_real, p_imag = pat[:modes, :], pat[modes:, :]
        i_real = cosine * p_real - sine * p_imag
        i_imag = cosine * p_imag + sine * p_real
        m_real, m_imag = mie_wide[:modes, lanes], mie_wide[modes:, lanes]
        inc[:modes, lanes] = i_real
        inc[modes:, lanes] = i_imag
        base[:modes, lanes] = m_real * i_real - m_imag * i_imag
        base[modes:, lanes] = m_real * i_imag + m_imag * i_real
    load_table.wait()
    for c in range(classes // 2):
        two = jnp.concatenate([table[2 * c], table[2 * c + 1]], 1)
        for k in range(2):
            part = two[k * modes : (k + 1) * modes].reshape(modes // ROWS, ROWS, both)
            matrix[:, k, :, c * both : (c + 1) * both] = part

    def share_copy(h, i, landing):
        at = lax.rem(group + groups - i, groups) if landing else group
        return pltpu.make_async_remote_copy(
            src_ref=recv.at[h, group],
            dst_ref=recv.at[h, at],
            send_sem=gsend_sem.at[h, i],
            recv_sem=grecv_sem.at[h, i],
            device_id={"groups": lax.rem(group + i, groups)},
            device_id_type=MESH,
        )

    def start_share(h):
        def end_slot(i, carry):
            copy = slot_copy(h, i, neighbour)
            copy.wait_send()
            copy.wait_recv()
            return carry

        def start_one(i, carry):
            share_copy(h, i, False).start()
            return carry

        lax.fori_loop(0, devices - 1, end_slot, 0)
        lax.fori_loop(1, groups, start_one, 0)

    def end_share(h):
        def end_one(i, carry):
            copy = share_copy(h, i, True)
            copy.wait_send()
            copy.wait_recv()
            return carry

        lax.fori_loop(1, groups, end_one, 0)

    for h in range(halvings):
        start_share(h)
    for h in range(halvings):
        end_share(h)

    def arrived(s, u):
        both_ranks = []
        for r in range(2):
            at = (2 * r + s) * units + u
            both_ranks.append(recv[at % share // bit, at // share, :, at % bit, :].astype(F32))
        return jnp.concatenate(both_ranks, 0)

    phases = []
    for s in range(2):
        for u in range(units - 1):
            c, t = divmod(u, whole)
            block = arrived(s, u).T.astype(BF16)
            if c < 2:
                groups_of = block.reshape(LANES // ROWS, ROWS, slots)
                at = slice(t * LANES // ROWS, (t + 1) * LANES // ROWS)
                left[s, at, c, :, 0:slots] = groups_of
                left[s, at, 1 - c, :, slots : 2 * slots] = -groups_of if c else groups_of
            else:
                rest = modes - whole * LANES
                at = slice(whole * LANES // ROWS, modes // ROWS)
                for c in range(2):
                    groups_of = block[c * rest : (c + 1) * rest].reshape(rest // ROWS, ROWS, slots)
                    left[s, at, c, :, 0:slots] = groups_of
                    left[s, at, 1 - c, :, slots : 2 * slots] = -groups_of if c else groups_of
        meta = arrived(s, units - 1)
        x, y, z = (
            meta[:, i : i + 1] + meta[:, PART + i : PART + i + 1] + meta[:, 2 * PART + i : 2 * PART + i + 1]
            for i in range(3)
        )
        phase = x * kx + y * ky + z * kz
        phases.append((jnp.cos(phase), jnp.sin(phase)))
    target = meta[:, TARGET_AT : TARGET_AT + 1]
    code = jnp.where(target > 0.0, meta[:, CLASS_AT : CLASS_AT + 1] * float(blocks) + target - 1.0, -1.0)
    code = jnp.broadcast_to(code, (slots, LANES))

    def form(c, n):
        rows = slice(c * modes, (c + 1) * modes) if isinstance(c, int) else pl.ds(pl.multiple_of(c * modes, 64), modes)
        for s in range(2):
            cosine, sine = phases[s]
            for t in range(2):
                first = (2 * n + t) * tile_blocks + c * blocks
                hit = code == (iota((slots, LANES), 1) // dirs + first).astype(F32)
                lanes = slice((2 * n + t) * LANES, (2 * n + t + 1) * LANES)
                weights[c, s, 0:slots, lanes] = jnp.where(hit, cosine, 0.0).astype(BF16)
                weights[c, s, slots : 2 * slots, lanes] = jnp.where(hit, sine, 0.0).astype(BF16)
            gathered = dot(left[s].reshape(both, 2 * slots), weights[c, s, :, n * WIDE : (n + 1) * WIDE])
            for t in range(2):
                g_real, g_imag = halves(gathered[:, t * LANES : (t + 1) * LANES])
                p_real, p_imag = pat[:modes, :], pat[modes:, :]
                at = (2 * n + t) * WIDE + s * LANES
                x_all[0, rows, at : at + LANES] = (g_real * p_real - g_imag * p_imag).astype(BF16)
                x_all[1, rows, at : at + LANES] = (g_real * p_imag + g_imag * p_real).astype(BF16)

    def form_first(c, carry):
        form(c, 0)
        return carry

    lax.fori_loop(0, classes, form_first, 0)

    def multiply(t):
        lanes = slice(t * WIDE, (t + 1) * WIDE)
        for k in range(2):
            z_buf[t % 2, k] = dot(matrix[...].reshape(both, classes * modes), x_all[k, :, lanes])

    def fold(t, ext):
        lanes = slice(t * WIDE, (t + 1) * WIDE)
        real_real, imag_real = halves(z_buf[t % 2, 0])
        real_imag, imag_imag = halves(z_buf[t % 2, 1])
        y_real = real_real - imag_imag
        y_imag = imag_real + real_imag
        m_real, m_imag = mie_wide[:modes, lanes], mie_wide[modes:, lanes]
        o_real = base[:modes, lanes] + (m_real * y_real - m_imag * y_imag)
        o_imag = base[modes:, lanes] + (m_real * y_imag + m_imag * y_real)
        out_ref[:modes, lanes] = o_real.astype(BF16)
        out_ref[modes:, lanes] = o_imag.astype(BF16)
        term = inc[:modes, lanes] * o_real + inc[modes:, lanes] * o_imag
        return ext + term.reshape(modes // 8, 8, WIDE).sum(0)

    ext = jnp.zeros((8, WIDE), F32)
    per_tile = classes // 2
    for t in range(tiles):
        multiply(t)
        if t < 2:
            for c in range(t * per_tile, (t + 1) * per_tile):
                form(c, 1)
        if t > 0:
            ext = fold(t - 1, ext)
    ext = fold(tiles - 1, ext)
    local = (ext[:, :LANES] + ext[:, LANES:]).sum(0, keepdims=True)
    ext_send[...] = local
    ext_recv[devices - 1] = local

    def ext_copy(number, to, here):
        return exchange(ext_send, ext_recv.at[here], esend_sem, erecv_sem, number, to)

    each_peer(lambda number, to: ext_copy(number, to, number).start())

    order_in, order_out = iota((WIDE, WIDE), 0), iota((WIDE, WIDE), 1)
    wanted = order_out // dirs % BLOCK * LANES + order_out // (BLOCK * dirs) * dirs + order_out % dirs
    shuffle = ones_where(order_in == wanted)
    stores = []
    for t in range(tiles):
        lanes = slice(t * WIDE, (t + 1) * WIDE)
        ordered[t] = dot(out_ref[:, lanes], shuffle).astype(BF16)
    for t in range(tiles):
        lanes = slice(t * WIDE, (t + 1) * WIDE)
        stores.append(pltpu.make_async_copy(ordered.at[t], out_hbm.at[:, lanes], out_sem.at[t]))
        stores[-1].start()
    for store in stores:
        store.wait()

    def end_ext(i, carry):
        copy = ext_copy(i, neighbour, i)
        copy.wait_send()
        copy.wait_recv()
        return carry

    lax.fori_loop(0, devices - 1, end_ext, 0)
    total = jnp.broadcast_to(ext_recv[...].sum(0), (8, LANES))
    shift = LANES // 2
    while shift >= dirs:
        total = total + pltpu.roll(total, shift, 1)
        shift //= 2
    ext_ref[...] = total[0:1, 0:dirs]


def hand_over(from_hbm, sums_hbm, to_hbm, ext_hbm, held, sums, in_sem, out_sem):
    count = held.shape[0]
    rows = held.shape[1]
    takes, gives = [], []
    for i in range(count):
        at = slice(i * rows, (i + 1) * rows)
        takes.append(pltpu.make_async_copy(from_hbm.at[at], held.at[i], in_sem.at[i]))
        gives.append(pltpu.make_async_copy(held.at[i], to_hbm.at[at], out_sem.at[i]))
    takes.append(pltpu.make_async_copy(sums_hbm, sums, in_sem.at[count]))
    gives.append(pltpu.make_async_copy(sums, ext_hbm, out_sem.at[count]))
    for take in takes:
        take.start()
    for take, give in zip(takes, gives):
        take.wait()
        give.start()
    for give in gives:
        give.wait()


def shards(
    positions, wave_vectors, pattern, dir_index, mie, trans_table, pair_route, pair_source, pair_target, pair_class,
):
    modes = pattern.shape[1]
    spheres = positions.shape[0]
    dirs = dir_index.shape[0]
    devices = lax.axis_size("sph")
    groups = lax.axis_size("groups")
    pairs = pair_source.shape[0]
    classes = trans_table.shape[0]
    both = 2 * modes
    columns = spheres * dirs
    units = both // LANES + 1
    share = 4 * units // groups
    waves = 2 if share % 2 == 0 else 1
    slots = 2 * devices
    vmem = pl.BlockSpec(memory_space=pltpu.VMEM)
    anywhere = pl.BlockSpec(memory_space=pl.ANY)
    dma = pltpu.SemaphoreType.DMA
    mixed, lane_sums = pl.pallas_call(
        body,
        out_shape=(
            jax.ShapeDtypeStruct((both, columns), BF16),
            jax.ShapeDtypeStruct((1, dirs), F32),
        ),
        in_specs=[anywhere] * 10,
        out_specs=(anywhere, vmem),
        scratch_shapes=[
            *[pltpu.VMEM((1, pairs), jnp.int32)] * 4,
            pltpu.VMEM((3, spheres), F32),
            pltpu.VMEM((3, wave_vectors.shape[0]), F32),
            pltpu.VMEM((1, dirs), jnp.int32),
            pltpu.VMEM((2, spheres, modes), F32),
            pltpu.VMEM((both, wave_vectors.shape[0]), F32),
            dma((9,)),
            pltpu.VMEM((both, columns), BF16),
            pltpu.VMEM((columns // WIDE, both, WIDE), BF16),
            dma((columns // WIDE,)),
            pltpu.VMEM((2, 2, both, WIDE), F32),
            pltpu.VMEM((waves, max(1, units // share), devices, share // waves, LANES), BF16),
            pltpu.VMEM((waves, groups, devices, share // waves, LANES), BF16),
            pltpu.VMEM((1, LANES), F32),
            pltpu.VMEM((devices, 1, LANES), F32),
            pltpu.VMEM((classes, both, modes), BF16),
            dma,
            dma((waves, devices)),
            dma((waves, devices)),
            dma((waves, groups)),
            dma((waves, groups)),
            dma((devices,)),
            dma((devices,)),
            pltpu.VMEM((LANES, spheres), F32),
            pltpu.VMEM((LANES, -(-modes // LANES) * LANES), F32),
            pltpu.VMEM((both, LANES), F32),
            pltpu.VMEM((both, columns), F32),
            pltpu.VMEM((both, columns), F32),
            pltpu.VMEM((both, columns), F32),
            pltpu.VMEM((2, modes // ROWS, 2, ROWS, 2 * slots), BF16),
            pltpu.VMEM((classes, 2, 2 * slots, columns // 2), BF16),
            pltpu.VMEM((modes // ROWS, 2, ROWS, classes * modes), BF16),
            pltpu.VMEM((2, classes * modes, columns), BF16),
        ],
        compiler_params=pltpu.CompilerParams(
            vmem_limit_bytes=63 * 1024 * 1024, collective_id=0, has_side_effects=True
        ),
        name="cluster",
    )(
        pair_route.reshape(1, pairs),
        pair_source[None],
        pair_target[None],
        pair_class[None],
        positions.T,
        wave_vectors.T,
        dir_index[None],
        mie.transpose(0, 2, 1),
        pattern.reshape(both, -1),
        trans_table.reshape(classes, both, modes),
    )
    pieces = 8
    scattered, extinction = pl.pallas_call(
        hand_over,
        out_shape=(
            jax.ShapeDtypeStruct((both, columns), BF16),
            jax.ShapeDtypeStruct((1, dirs), F32),
        ),
        in_specs=[anywhere, anywhere],
        out_specs=(anywhere, anywhere),
        scratch_shapes=[
            pltpu.VMEM((pieces, both // pieces, columns), BF16),
            pltpu.VMEM((1, dirs), F32),
            dma((pieces + 1,)),
            dma((pieces + 1,)),
        ],
        compiler_params=pltpu.CompilerParams(vmem_limit_bytes=63 * 1024 * 1024),
        name="hand_over",
    )(mixed, lane_sums)
    return (scattered, extinction[0])


def solution(mesh):
    placed = (
        P("sph", None),
        P(),
        P(),
        P("groups"),
        P(None, None, "sph"),
        P(),
        P("sph", None),
        P("sph"),
        P("sph"),
        P("sph"),
    )
    return jax.shard_map(
        shards,
        mesh=mesh,
        in_specs=placed,
        out_specs=(P(None, ("groups", "sph")), P("groups")),
        check_vma=False,
    )
```

```python
import jax
import jax.numpy as jnp
from jax import lax
from jax.experimental import pallas as pl
from jax.experimental.pallas import tpu as pltpu
from jax.sharding import PartitionSpec as P

BLOCK = 2
LANES = 128
WIDE = 256
PART = 8
TARGET_AT = 24
CLASS_AT = 25
F32 = jnp.float32
BF16 = jnp.bfloat16
HIGHEST = lax.Precision.HIGHEST
MESH = pl.DeviceIdType.MESH
NT = (((1,), (1,)), ((), ()))


def iota(shape, axis):
    return lax.broadcasted_iota(jnp.int32, shape, axis)


def ones_where(mask):
    return mask.astype(F32).astype(BF16)


def split3(x):
    hi = x.astype(BF16)
    rest = x - hi.astype(F32)
    mid = rest.astype(BF16)
    low = (rest - mid.astype(F32)).astype(BF16)
    return hi, mid, low


def dot(a, b, **kw):
    return jnp.dot(a, b, preferred_element_type=F32, **kw)


ROWS = 16


def paired(x):
    return x.reshape(x.shape[0] // (2 * ROWS), 2, ROWS, x.shape[1])


def halves(x):
    groups = paired(x)
    flat = (x.shape[0] // 2, x.shape[1])
    return groups[:, 0].reshape(flat), groups[:, 1].reshape(flat)


def body(
    route_hbm, source_hbm, target_hbm, class_hbm, pos_hbm, wave_hbm, dirs_hbm, mie_hbm, pattern_hbm, table_hbm,
    out_hbm, ext_ref,
    route_ref, source_ref, target_ref, class_ref, pos_ref, wave_ref, dirs_ref, mie_ref, pattern_ref, load_sem,
    out_ref, ordered, out_sem, z_buf,
    send, recv, ext_send, ext_mid, near_recv, ext_recv, table, table_sem, send_sem, recv_sem, gsend_sem, grecv_sem, esend_sem, erecv_sem,
    parts, mie_rows, pat, mie_wide, inc, base, left, weights, matrix, x_all,
):
    me = lax.axis_index("sph")
    group = lax.axis_index("groups")
    devices = lax.axis_size("sph")
    groups = lax.axis_size("groups")
    pairs = route_ref.shape[1]
    spheres, modes = mie_ref.shape[1:]
    both = 2 * modes
    classes = table.shape[0]
    columns = out_ref.shape[1]
    dirs = dirs_ref.shape[1]
    blocks = spheres // BLOCK
    tile_blocks = LANES // dirs
    tiles = blocks // tile_blocks
    slots = 2 * devices
    units = both // LANES + 1
    share = recv.shape[2]
    whole = modes // LANES

    barrier = pltpu.get_barrier_semaphore()

    middle = devices // 2
    stride = 5

    def each_peer(act):
        def pair(e):
            for number, offset in ((2 * e, middle - e), (2 * e + 1, middle + 1 + e)):
                to = me + offset
                act(number, jnp.where(to >= devices, to - devices, to))

        def some(j, carry):
            for u in range(stride):
                pair(j * stride + u)
            return carry

        lax.fori_loop(0, (middle - 1) // stride, some, 0)
        for e in range((middle - 1) // stride * stride, middle - 1):
            pair(e)
        to = me + 1
        act(devices - 2, jnp.where(to >= devices, to - devices, to))

    def greet(number, to):
        pl.semaphore_signal(barrier, inc=1, device_id={"sph": to}, device_id_type=MESH)

    def greet_group(i, carry):
        pl.semaphore_signal(barrier, inc=1, device_id={"groups": lax.rem(group + i, groups)}, device_id_type=MESH)
        return carry

    each_peer(greet)
    lax.fori_loop(1, groups, greet_group, 0)
    given = (route_hbm, source_hbm, target_hbm, class_hbm, pos_hbm, mie_hbm, wave_hbm, dirs_hbm, pattern_hbm)
    taken = (route_ref, source_ref, target_ref, class_ref, pos_ref, mie_ref, wave_ref, dirs_ref, pattern_ref)
    loads = [pltpu.make_async_copy(a, b, load_sem.at[i]) for i, (a, b) in enumerate(zip(given, taken))]
    load_table = pltpu.make_async_copy(table_hbm, table, table_sem)
    for load in loads:
        load.start()
    load_table.start()
    for load in loads[:6]:
        load.wait()

    named = ones_where(route_ref[...] == iota((devices, pairs), 0))
    earlier = ones_where(iota((pairs, pairs), 0) < iota((pairs, pairs), 1))
    before = dot(named, earlier)
    parts[...] = jnp.zeros_like(parts)
    for i, part in enumerate(split3(pos_ref[...])):
        parts[i * PART : i * PART + 3, :] = part.astype(F32)
    row = iota((LANES, pairs), 0)
    pair_meta = jnp.where(
        row == TARGET_AT, target_ref[...] + 1, jnp.where(row == CLASS_AT, class_ref[...], 0)
    ).astype(F32).astype(BF16)
    mixed = jnp.concatenate([mie_ref[0, :, whole * LANES :], mie_ref[1, :, whole * LANES :]], 1)
    first_unit = group * share
    rows_of_share = max(1, share // units)
    for n in range(rows_of_share):
        kind = first_unit // units + n
        rank = (kind // 2).astype(F32)
        sphere = lax.rem(kind, 2)
        slot = jnp.where(before == rank, named.astype(F32), 0.0).astype(BF16)
        origin = ones_where(source_ref[...] * BLOCK + sphere == iota((spheres, pairs), 0))
        pick = lax.dot_general(slot, origin, NT, preferred_element_type=F32).astype(BF16)
        meta = lax.dot_general(slot, pair_meta, NT, preferred_element_type=F32)
        where = lax.dot_general(pick, parts[...].astype(BF16), NT, preferred_element_type=F32)
        for u in range(units):
            if u == units - 1:
                value = where + meta
            else:
                c, t = divmod(u, whole)
                rows = mixed if c == 2 else mie_ref[c, :, t * LANES : (t + 1) * LANES]
                value = dot(pick, rows.astype(BF16))
            at = n * units + u
            send[at // share, :, at % share, :] = value.astype(BF16)
    piece = lax.rem(first_unit, units) // share if share < units else 0

    pl.semaphore_wait(barrier, devices + groups - 2)

    def exchange(src, dst, sends, receives, number, to):
        return pltpu.make_async_remote_copy(
            src_ref=src,
            dst_ref=dst,
            send_sem=sends.at[number],
            recv_sem=receives.at[number],
            device_id={"sph": to},
            device_id_type=MESH,
        )

    neighbour = jnp.where(me + 1 >= devices, 0, me + 1)

    def slot_copy(number, to):
        return exchange(send.at[piece, to], recv.at[group, number], send_sem, recv_sem, number, to)

    each_peer(lambda number, to: slot_copy(number, to).start())
    recv[group, devices - 1] = send[piece, me]
    for load in loads[6:]:
        load.wait()

    lane_dir = dirs_ref[...]
    lane_dirs = jnp.concatenate([lane_dir] * tile_blocks, 1)
    select = (iota((pattern_ref.shape[1], LANES), 0) == lane_dirs).astype(F32)
    pat[...] = dot(pattern_ref[...], select, precision=HIGHEST)
    waves = dot(wave_ref[...], select, precision=HIGHEST)
    kx, ky, kz = waves[0:1], waves[1:2], waves[2:3]
    wide = iota((LANES, columns), 1)
    sphere_of = ((wide // WIDE) * tile_blocks + wide // dirs % tile_blocks) * BLOCK + wide // LANES % BLOCK
    spread = ones_where(lax.rem(iota((LANES, columns), 0), spheres) == sphere_of)
    own = dot(pos_ref[...], spread[0:spheres].astype(F32), precision=HIGHEST)
    mie_rows[...] = jnp.zeros_like(mie_rows)
    for c in range(2):
        for i, part in enumerate(split3(mie_ref[c])):
            mie_rows[i * spheres : (i + 1) * spheres, 0:modes] = part.astype(F32)
        mie_wide[c * modes : (c + 1) * modes, :] = dot(mie_rows[...].T[:modes].astype(BF16), spread)
    for n in range(columns // LANES):
        lanes = slice(n * LANES, (n + 1) * LANES)
        phase = own[0:1, lanes] * kx + own[1:2, lanes] * ky + own[2:3, lanes] * kz
        cosine, sine = jnp.cos(phase), jnp.sin(phase)
        p_real, p_imag = pat[:modes, :], pat[modes:, :]
        i_real = cosine * p_real - sine * p_imag
        i_imag = cosine * p_imag + sine * p_real
        m_real, m_imag = mie_wide[:modes, lanes], mie_wide[modes:, lanes]
        inc[:modes, lanes] = i_real
        inc[modes:, lanes] = i_imag
        base[:modes, lanes] = m_real * i_real - m_imag * i_imag
        base[modes:, lanes] = m_real * i_imag + m_imag * i_real
    load_table.wait()
    for c in range(classes // 2):
        two = jnp.concatenate([table[2 * c], table[2 * c + 1]], 1)
        for k in range(2):
            part = two[k * modes : (k + 1) * modes].reshape(modes // ROWS, ROWS, both)
            matrix[:, k, :, c * both : (c + 1) * both] = part

    def end_slot(i, carry):
        copy = slot_copy(i, neighbour)
        copy.wait_send()
        copy.wait_recv()
        return carry

    quarter = devices // 4

    def share_copy(q, i, landing):
        at = lax.rem(group + groups - i, groups) if landing else group
        rows = pl.ds(q * quarter, quarter)
        return pltpu.make_async_remote_copy(
            src_ref=recv.at[group, rows],
            dst_ref=recv.at[at, rows],
            send_sem=gsend_sem.at[q, i],
            recv_sem=grecv_sem.at[q, i],
            device_id={"groups": lax.rem(group + i, groups)},
            device_id_type=MESH,
        )

    def start_share(q):
        lax.fori_loop(q * quarter, min((q + 1) * quarter, devices - 1), end_slot, 0)

        def start_one(i, carry):
            share_copy(q, i, False).start()
            return carry

        lax.fori_loop(1, groups, start_one, 0)

    def end_share(q, carry):
        def end_one(i, carry):
            copy = share_copy(q, i, True)
            copy.wait_send()
            copy.wait_recv()
            return carry

        return lax.fori_loop(1, groups, end_one, carry)

    for q in (3, 0, 2, 1):
        start_share(q)
    lax.fori_loop(0, 4, end_share, 0)

    def arrived(s, u):
        both_ranks = []
        for r in range(2):
            at = (2 * r + s) * units + u
            both_ranks.append(recv[at // share, :, at % share, :].astype(F32))
        return jnp.concatenate(both_ranks, 0)

    phases = []
    for s in range(2):
        for u in range(units - 1):
            c, t = divmod(u, whole)
            block = arrived(s, u).T.astype(BF16)
            if c < 2:
                groups_of = block.reshape(LANES // ROWS, ROWS, slots)
                at = slice(t * LANES // ROWS, (t + 1) * LANES // ROWS)
                left[s, at, c, :, 0:slots] = groups_of
                left[s, at, 1 - c, :, slots : 2 * slots] = -groups_of if c else groups_of
            else:
                rest = modes - whole * LANES
                at = slice(whole * LANES // ROWS, modes // ROWS)
                for c in range(2):
                    groups_of = block[c * rest : (c + 1) * rest].reshape(rest // ROWS, ROWS, slots)
                    left[s, at, c, :, 0:slots] = groups_of
                    left[s, at, 1 - c, :, slots : 2 * slots] = -groups_of if c else groups_of
        meta = arrived(s, units - 1)
        x, y, z = (
            meta[:, i : i + 1] + meta[:, PART + i : PART + i + 1] + meta[:, 2 * PART + i : 2 * PART + i + 1]
            for i in range(3)
        )
        phase = x * kx + y * ky + z * kz
        phases.append((jnp.cos(phase), jnp.sin(phase)))
    target = meta[:, TARGET_AT : TARGET_AT + 1]
    code = jnp.where(target > 0.0, meta[:, CLASS_AT : CLASS_AT + 1] * float(blocks) + target - 1.0, -1.0)
    code = jnp.broadcast_to(code, (slots, LANES))

    def form(c, n):
        rows = slice(c * modes, (c + 1) * modes) if isinstance(c, int) else pl.ds(pl.multiple_of(c * modes, 64), modes)
        for s in range(2):
            cosine, sine = phases[s]
            for t in range(2):
                first = (2 * n + t) * tile_blocks + c * blocks
                hit = code == (iota((slots, LANES), 1) // dirs + first).astype(F32)
                lanes = slice((2 * n + t) * LANES, (2 * n + t + 1) * LANES)
                weights[c, s, 0:slots, lanes] = jnp.where(hit, cosine, 0.0).astype(BF16)
                weights[c, s, slots : 2 * slots, lanes] = jnp.where(hit, sine, 0.0).astype(BF16)
            gathered = dot(left[s].reshape(both, 2 * slots), weights[c, s, :, n * WIDE : (n + 1) * WIDE])
            for t in range(2):
                g_real, g_imag = halves(gathered[:, t * LANES : (t + 1) * LANES])
                p_real, p_imag = pat[:modes, :], pat[modes:, :]
                at = (2 * n + t) * WIDE + s * LANES
                x_all[0, rows, at : at + LANES] = (g_real * p_real - g_imag * p_imag).astype(BF16)
                x_all[1, rows, at : at + LANES] = (g_real * p_imag + g_imag * p_real).astype(BF16)

    def form_first(c, carry):
        form(c, 0)
        return carry

    lax.fori_loop(0, classes, form_first, 0)

    def multiply(t):
        lanes = slice(t * WIDE, (t + 1) * WIDE)
        for k in range(2):
            z_buf[t % 2, k] = dot(matrix[...].reshape(both, classes * modes), x_all[k, :, lanes])

    def fold(t, ext):
        lanes = slice(t * WIDE, (t + 1) * WIDE)
        real_real, imag_real = halves(z_buf[t % 2, 0])
        real_imag, imag_imag = halves(z_buf[t % 2, 1])
        y_real = real_real - imag_imag
        y_imag = imag_real + real_imag
        m_real, m_imag = mie_wide[:modes, lanes], mie_wide[modes:, lanes]
        o_real = base[:modes, lanes] + (m_real * y_real - m_imag * y_imag)
        o_imag = base[modes:, lanes] + (m_real * y_imag + m_imag * y_real)
        out_ref[:modes, lanes] = o_real.astype(BF16)
        out_ref[modes:, lanes] = o_imag.astype(BF16)
        term = inc[:modes, lanes] * o_real + inc[modes:, lanes] * o_imag
        return ext + term.reshape(modes // 8, 8, WIDE).sum(0)

    ext = jnp.zeros((8, WIDE), F32)
    per_tile = classes // 2
    for t in range(tiles):
        multiply(t)
        if t < 2:
            for c in range(t * per_tile, (t + 1) * per_tile):
                form(c, 1)
        if t > 0:
            ext = fold(t - 1, ext)
    ext = fold(tiles - 1, ext)
    local = (ext[:, :LANES] + ext[:, LANES:]).sum(0, keepdims=True)
    near, far = near_recv.shape[0], ext_recv.shape[0]
    first = me // near * near

    def near_copy(i):
        return exchange(ext_send, near_recv.at[i], esend_sem, erecv_sem, i, first + lax.rem(me + i, near))

    def far_copy(i):
        to = me + near * i
        to = jnp.where(to >= devices, to - devices, to)
        return exchange(ext_mid, ext_recv.at[i], esend_sem, erecv_sem, near + i, to)

    ext_send[...] = local
    near_recv[0] = local
    for i in range(1, near):
        near_copy(i).start()
    for i in range(1, near):
        copy = near_copy(i)
        copy.wait_send()
        copy.wait_recv()
    gathered = near_recv[...].sum(0)
    ext_mid[...] = gathered
    ext_recv[0] = gathered
    for i in sorted(range(1, far), key=lambda i: abs(i - far // 2)):
        far_copy(i).start()

    order_in, order_out = iota((WIDE, WIDE), 0), iota((WIDE, WIDE), 1)
    wanted = order_out // dirs % BLOCK * LANES + order_out // (BLOCK * dirs) * dirs + order_out % dirs
    shuffle = ones_where(order_in == wanted)
    stores = []
    for t in range(tiles):
        lanes = slice(t * WIDE, (t + 1) * WIDE)
        ordered[t] = dot(out_ref[:, lanes], shuffle).astype(BF16)
    for t in range(tiles):
        lanes = slice(t * WIDE, (t + 1) * WIDE)
        stores.append(pltpu.make_async_copy(ordered.at[t], out_hbm.at[:, lanes], out_sem.at[t]))
        stores[-1].start()
    for store in stores:
        store.wait()

    for i in range(1, far):
        copy = far_copy(i)
        copy.wait_send()
        copy.wait_recv()
    total = jnp.broadcast_to(ext_recv[...].sum(0), (8, LANES))
    shift = LANES // 2
    while shift >= dirs:
        total = total + pltpu.roll(total, shift, 1)
        shift //= 2
    ext_ref[...] = total[0:1, 0:dirs]


def hand_over(from_hbm, sums_hbm, to_hbm, ext_hbm, held, sums, in_sem, out_sem):
    count = held.shape[0]
    rows = held.shape[1]
    takes, gives = [], []
    for i in range(count):
        at = slice(i * rows, (i + 1) * rows)
        takes.append(pltpu.make_async_copy(from_hbm.at[at], held.at[i], in_sem.at[i]))
        gives.append(pltpu.make_async_copy(held.at[i], to_hbm.at[at], out_sem.at[i]))
    takes.append(pltpu.make_async_copy(sums_hbm, sums, in_sem.at[count]))
    gives.append(pltpu.make_async_copy(sums, ext_hbm, out_sem.at[count]))
    for take in takes:
        take.start()
    for take, give in zip(takes, gives):
        take.wait()
        give.start()
    for give in gives:
        give.wait()


def shards(
    positions, wave_vectors, pattern, dir_index, mie, trans_table, pair_route, pair_source, pair_target, pair_class,
):
    modes = pattern.shape[1]
    spheres = positions.shape[0]
    dirs = dir_index.shape[0]
    devices = lax.axis_size("sph")
    groups = lax.axis_size("groups")
    pairs = pair_source.shape[0]
    classes = trans_table.shape[0]
    both = 2 * modes
    columns = spheres * dirs
    units = both // LANES + 1
    share = 4 * units // groups
    slots = 2 * devices
    near = 4
    vmem = pl.BlockSpec(memory_space=pltpu.VMEM)
    anywhere = pl.BlockSpec(memory_space=pl.ANY)
    dma = pltpu.SemaphoreType.DMA
    mixed, lane_sums = pl.pallas_call(
        body,
        out_shape=(
            jax.ShapeDtypeStruct((both, columns), BF16),
            jax.ShapeDtypeStruct((1, dirs), F32),
        ),
        in_specs=[anywhere] * 10,
        out_specs=(anywhere, vmem),
        scratch_shapes=[
            *[pltpu.VMEM((1, pairs), jnp.int32)] * 4,
            pltpu.VMEM((3, spheres), F32),
            pltpu.VMEM((3, wave_vectors.shape[0]), F32),
            pltpu.VMEM((1, dirs), jnp.int32),
            pltpu.VMEM((2, spheres, modes), F32),
            pltpu.VMEM((both, wave_vectors.shape[0]), F32),
            dma((9,)),
            pltpu.VMEM((both, columns), BF16),
            pltpu.VMEM((columns // WIDE, both, WIDE), BF16),
            dma((columns // WIDE,)),
            pltpu.VMEM((2, 2, both, WIDE), F32),
            pltpu.VMEM((max(1, units // share), devices, share, LANES), BF16),
            pltpu.VMEM((groups, devices, share, LANES), BF16),
            pltpu.VMEM((1, LANES), F32),
            pltpu.VMEM((1, LANES), F32),
            pltpu.VMEM((near, 1, LANES), F32),
            pltpu.VMEM((devices // near, 1, LANES), F32),
            pltpu.VMEM((classes, both, modes), BF16),
            dma,
            dma((devices,)),
            dma((devices,)),
            dma((4, groups)),
            dma((4, groups)),
            dma((devices,)),
            dma((devices,)),
            pltpu.VMEM((LANES, spheres), F32),
            pltpu.VMEM((LANES, -(-modes // LANES) * LANES), F32),
            pltpu.VMEM((both, LANES), F32),
            pltpu.VMEM((both, columns), F32),
            pltpu.VMEM((both, columns), F32),
            pltpu.VMEM((both, columns), F32),
            pltpu.VMEM((2, modes // ROWS, 2, ROWS, 2 * slots), BF16),
            pltpu.VMEM((classes, 2, 2 * slots, columns // 2), BF16),
            pltpu.VMEM((modes // ROWS, 2, ROWS, classes * modes), BF16),
            pltpu.VMEM((2, classes * modes, columns), BF16),
        ],
        compiler_params=pltpu.CompilerParams(
            vmem_limit_bytes=63 * 1024 * 1024, collective_id=0, has_side_effects=True
        ),
        name="cluster",
    )(
        pair_route.reshape(1, pairs),
        pair_source[None],
        pair_target[None],
        pair_class[None],
        positions.T,
        wave_vectors.T,
        dir_index[None],
        mie.transpose(0, 2, 1),
        pattern.reshape(both, -1),
        trans_table.reshape(classes, both, modes),
    )
    pieces = 8
    scattered, extinction = pl.pallas_call(
        hand_over,
        out_shape=(
            jax.ShapeDtypeStruct((both, columns), BF16),
            jax.ShapeDtypeStruct((1, dirs), F32),
        ),
        in_specs=[anywhere, anywhere],
        out_specs=(anywhere, anywhere),
        scratch_shapes=[
            pltpu.VMEM((pieces, both // pieces, columns), BF16),
            pltpu.VMEM((1, dirs), F32),
            dma((pieces + 1,)),
            dma((pieces + 1,)),
        ],
        compiler_params=pltpu.CompilerParams(vmem_limit_bytes=63 * 1024 * 1024),
        name="hand_over",
    )(mixed, lane_sums)
    return (scattered, extinction[0])


def solution(mesh):
    placed = (
        P("sph", None),
        P(),
        P(),
        P("groups"),
        P(None, None, "sph"),
        P(),
        P("sph", None),
        P("sph"),
        P("sph"),
        P("sph"),
    )
    return jax.shard_map(
        shards,
        mesh=mesh,
        in_specs=placed,
        out_specs=(P(None, ("groups", "sph")), P("groups")),
        check_vma=False,
    )
```
